128 devices in a mesh: dp: 4 (over z), mp: 32 (over y, x, core).
Axes of the slice: x: 4, y: 4, z: 4, core: 2. Of those that a mesh axis runs over, the one named last changes fastest.
Arguments:
- tokens: bfloat16 [4096, 4096], P('dp', 'mp'), may hold values from -6 to 6
- decay: float32 [4096, 16], P('dp'), may hold values from 0.75 to 1, as said below
- state: float32 [128, 256, 8192], P('dp', None, 'mp'), may hold values from -24 to 24
- w_query: bfloat16 [4096, 4096], P(None, 'mp'), may hold values from -0.09375 to 0.09375
- w_key: bfloat16 [4096, 4096], P(None, 'mp'), may hold values from -0.09375 to 0.09375
- w_value: bfloat16 [4096, 8192], P(None, 'mp'), may hold values from -0.09375 to 0.09375
- w_gate: bfloat16 [4096, 8192], P(None, 'mp'), may hold values from -0.09375 to 0.09375
- w_out: bfloat16 [8192, 4096], P('mp'), may hold values from -0.125 to 0.125
- norm_gain: float32 [8192], P('mp'), may hold values from 0.25 to 1.75
Outputs:
- layer_out: bfloat16 [4096, 4096], P('dp', 'mp')
- new_state: float32 [128, 256, 8192], P('dp', None, 'mp')
The draws below stay inside these ranges and needn't reach their ends.
Inputs may be any that keep to these rules, and one draw needn't show every extreme that they name: `decay`: each head has its own base rate over all tokens, varied somewhat from token to token.
All inputs are finite; a program needn't handle non-finite values.
Results may differ from the reference program's by a relative error of at most 0.0071.
Values may be sent and summed in bfloat16 or wider, within the bound.
A program may use at most 128 MiB of HBM per device.

```python
import jax
import jax.numpy as jnp
from jax import lax

D = 4096
H = 16
HEAD = 256
VHEAD = 512
NEW = 32
BATCH = 128
TOKENS = 4096


def draw_decay(key, part):
    base_key, jitter_key = jax.random.split(key)
    base_low = 0.85
    jitter_low = 0.93
    base_rate = jnp.exp(jax.random.uniform(base_key, (H,), jnp.float32, jnp.log(base_low), jnp.log(0.999)))
    jitter = jax.random.uniform(jitter_key, (TOKENS, H), jnp.float32, jitter_low, 1.0)
    return base_rate[None, :] * jitter


def with_spikes(result, key, source, target, parts, factor):
    owner, partner = [(jnp.arange(result.shape[position]) // (result.shape[position] // parts)).reshape([-1 if axis == position else 1 for axis in range(result.ndim)]) for position in (source, target)]
    chosen = jax.random.permutation(key, parts)[partner]
    strong = (owner == chosen) | (owner == (partner + parts // 2) % parts)
    return jnp.where(strong, factor * result, result)


def block_levels(rng, dims, shards, low, largest):
    level = 1.0
    for position, shards_of in shards:
        heights = jax.random.uniform(jax.random.fold_in(jax.random.fold_in(rng, 6), position), (shards_of,), jnp.float32, low / len(shards), largest / len(shards))
        level = level * jnp.repeat(jnp.exp(heights), dims[position] // shards_of).reshape((-1,) + (1,) * (len(dims) - 1 - position))
    return level


def gaussian(rng, shape, scale, most, cuts=(), held_as=jnp.bfloat16):
    values = scale * jax.random.normal(rng, shape, jnp.float32)
    if cuts:
        values = values * block_levels(rng, shape, cuts, -0.22, 0.18)
    return jnp.clip(values, -most, most).astype(held_as)


def bell_draw_with(own_key, shape, width, most, pieces, heavy, held_as=jnp.bfloat16):
    result = width * jax.random.normal(own_key, shape, jnp.float32)
    if pieces:
        result = result * block_levels(own_key, shape, pieces, -0.22, 0.18)
    return jnp.clip(with_spikes(result, jax.random.fold_in(own_key, 3), *heavy), -most, most).astype(held_as)


def setup_inputs(seed: int = 0) -> dict:
    arg_keys = jax.random.split(jax.random.key(seed), 10)
    return {
        "tokens": gaussian(arg_keys[0], (TOKENS, D), 1.0, 6.0, ((0, 4), (1, 32))),
        "decay": draw_decay(jax.random.fold_in(arg_keys[9], 71), 0),
        "state": gaussian(arg_keys[2], (BATCH, HEAD, H * VHEAD), 4.0, 24.0, ((0, 4), (2, 32)), jnp.float32),
        "w_query": gaussian(arg_keys[3], (D, H * HEAD), D ** -0.5, 0.09375, ((1, 32),)),
        "w_key": gaussian(arg_keys[4], (D, H * HEAD), D ** -0.5, 0.09375, ((1, 32),)),
        "w_value": gaussian(arg_keys[5], (D, H * VHEAD), D ** -0.5, 0.09375, ((1, 32),)),
        "w_gate": gaussian(arg_keys[6], (D, H * VHEAD), D ** -0.5, 0.09375, ((1, 32),)),
        "w_out": bell_draw_with(arg_keys[7], (H * VHEAD, D), (H * VHEAD) ** -0.5, 0.125, ((0, 32),), (0, 1, 32, 2.75)),
        "norm_gain": jnp.clip(1.0 + 0.15 * jax.random.normal(arg_keys[8], (H * VHEAD,), jnp.float32), 0.25, 1.75),
    }


EPS = 0.1

def one_sequence(packed):
    query, key_proj, value_proj, decay_rates, old_state = packed
    highest = lax.Precision.HIGHEST
    log_cumul = jnp.cumsum(jnp.log(decay_rates), axis=0)
    from_state = jnp.einsum('nhk,khv->nhv', query.astype(jnp.float32), old_state, precision=highest)
    scores = jnp.einsum('nhk,mhk->hnm', query.astype(jnp.float32), key_proj.astype(jnp.float32), precision=highest)
    along = log_cumul.T
    log_gap = along[:, :, None] - along[:, None, :]
    causal = jnp.arange(NEW)[:, None] >= jnp.arange(NEW)[None, :]
    factor = jnp.where(causal, jnp.exp(jnp.where(causal, log_gap, 0.0)), 0.0)
    weights = (scores * factor).astype(jnp.bfloat16)
    in_block = jnp.einsum('hnm,mhv->nhv', weights.astype(jnp.float32), value_proj.astype(jnp.float32), precision=highest)
    retained = jnp.exp(log_cumul)[:, :, None] * from_state + in_block
    final_log = log_cumul[-1]
    carry_scale = jnp.exp(final_log[None, :] - log_cumul)
    decayed_keys = key_proj.astype(jnp.float32) * carry_scale[:, :, None]
    fresh = jnp.einsum('nhk,nhv->khv', decayed_keys, value_proj.astype(jnp.float32), precision=highest)
    new_state = jnp.exp(final_log)[None, :, None] * old_state + fresh
    return (retained, new_state)

def reference(tokens, decay, state, w_query, w_key, w_value, w_gate, w_out, norm_gain):
    query = (jnp.dot(tokens, w_query, preferred_element_type=jnp.float32) * HEAD ** (-0.5)).astype(jnp.bfloat16)
    key_proj = jnp.dot(tokens, w_key, preferred_element_type=jnp.float32).astype(jnp.bfloat16)
    value_proj = jnp.dot(tokens, w_value, preferred_element_type=jnp.float32).astype(jnp.bfloat16)
    gate_proj = jnp.dot(tokens, w_gate, preferred_element_type=jnp.float32)
    packed = (query.reshape(BATCH, NEW, H, HEAD), key_proj.reshape(BATCH, NEW, H, HEAD), value_proj.reshape(BATCH, NEW, H, VHEAD), decay.reshape(BATCH, NEW, H), state.reshape(BATCH, HEAD, H, VHEAD))
    retained, new_state = lax.map(one_sequence, packed)
    retained = retained.reshape(TOKENS, H, VHEAD)
    centre = lax.optimization_barrier(jnp.mean(retained, axis=-1))
    deviation = retained - centre[..., None]
    variance = lax.optimization_barrier(jnp.mean(deviation * deviation, axis=-1))
    normed = deviation * lax.rsqrt(variance + EPS)[..., None]
    gated_out = (normed.reshape(TOKENS, H * VHEAD) * norm_gain * jax.nn.silu(gate_proj)).astype(jnp.bfloat16)
    layer_out = jnp.dot(gated_out, w_out, preferred_element_type=jnp.float32).astype(jnp.bfloat16)
    return (layer_out, new_state.reshape(BATCH, HEAD, H * VHEAD))
```

```python
import functools

import jax
import jax.numpy as jnp
from jax import lax
from jax.experimental import pallas as pl
from jax.experimental.pallas import tpu as pltpu
from jax.sharding import PartitionSpec as P

HEAD = 256
VHEAD = 512
NEW = 32
EPS = 0.1
SIDE = 4
CHIPS = SIDE * SIDE
BLOCK = 128

MESH = pl.DeviceIdType.MESH
HIGHEST = lax.Precision.HIGHEST
BF16 = jnp.bfloat16
F32 = jnp.float32


class Place:
    def __init__(self):
        self.me = lax.axis_index("mp")
        self.core = lax.rem(self.me, 2)
        chip = lax.div(self.me, 2)
        y, x = lax.div(chip, SIDE), lax.rem(chip, SIDE)
        self.a = x * (1 - self.core) + y * self.core
        self.b = y * (1 - self.core) + x * self.core
        self.step_a = 1 + (SIDE - 1) * self.core
        self.step_b = SIDE - (SIDE - 1) * self.core
        self.partner = self.me + 1 - 2 * self.core

    def chip(self, da, db):
        a = lax.rem(self.a + (da + SIDE), SIDE)
        b = lax.rem(self.b + (db + SIDE), SIDE)
        return a * self.step_a + b * self.step_b

    def at(self, da, db):
        return self.chip(da, db) * 2 + self.core

    def partner_at(self, da, db):
        a = lax.rem(self.b + (da + SIDE), SIDE)
        b = lax.rem(self.a + (db + SIDE), SIDE)
        return (a * self.step_b + b * self.step_a) * 2 + 1 - self.core


def remote(src, dst, send_sem, recv_sem, device):
    return pltpu.make_async_remote_copy(
        src_ref=src,
        dst_ref=dst,
        send_sem=send_sem,
        recv_sem=recv_sem,
        device_id={"mp": device},
        device_id_type=MESH,
    )


def greet(place):
    barrier = pltpu.get_barrier_semaphore()
    others = (place.partner, place.at(1, 0), place.at(-1, 0), place.at(0, 1), place.at(0, -1))
    for other in others:
        pl.semaphore_signal(barrier, inc=1, device_id={"mp": other}, device_id_type=MESH)
    pl.semaphore_wait(barrier, len(others))


ARRIVALS = (
    ((-1, 0, 0), (1, 0, 0), (0, -1, 0), (0, 1, 0)),
    ((-1, 0, 1), (1, 0, 1)),
    ((0, -1, 1), (0, 1, 1)),
    ((-1, -1, 0), (-1, 1, 0), (1, -1, 0), (1, 1, 0), (2, 0, 0), (2, 0, 1), (0, 2, 0), (0, 2, 1)),
    ((-1, -1, 1), (-1, 1, 1)),
    ((1, -1, 1), (1, 1, 1)),
    ((2, -1, 0), (2, 1, 0), (2, -1, 1), (2, 1, 1)),
    ((-1, 2, 0), (-1, 2, 1), (1, 2, 0), (1, 2, 1)),
    ((2, 2, 0), (2, 2, 1)),
)
PAIRS = {
    1: ((-1, 0), (1, 0)),
    2: ((0, -1), (0, 1)),
    3: ((2, 0), (0, 2)),
    4: ((-1, -1), (-1, 1)),
    5: ((1, -1), (1, 1)),
    6: ((2, -1), (2, 1)),
    7: ((-1, 2), (1, 2)),
}


def gather_kernel(
    tokens, w_query, w_key, w_value, w_gate, w_out,
    query, key_proj, value_proj, gate_proj, other_out,
    held, weights, total, send_sems, recv_sems, side_sems, local_sems,
):
    place = Place()
    rows = tokens.shape[0]
    sub = rows // 2
    me, core, partner = place.me, place.core, place.partner
    sent = []

    def rows_of(half):
        return pl.ds(half * sub, sub)

    def send(src, block, half, device):
        copy = remote(
            src, held.at[block, rows_of(half)], send_sems.at[len(sent)], recv_sems.at[block, half], device
        )
        copy.start()
        sent.append(copy)

    greet(place)
    ring = (place.at(1, 0), place.at(-1, 0), place.at(0, 1), place.at(0, -1))
    a_up, a_down, b_up, b_down = ring
    for half in range(2):
        for device in ring + (partner,):
            send(tokens.at[rows_of(half)], me, half, device)
    mine = pl.ds(pl.multiple_of(core * BLOCK, BLOCK), BLOCK)
    loads = [
        pltpu.make_async_copy(tokens, held.at[me], local_sems.at[0]),
        pltpu.make_async_copy(w_query, weights.at[0, :, mine], local_sems.at[1]),
        pltpu.make_async_copy(w_key, weights.at[1, :, mine], local_sems.at[2]),
        pltpu.make_async_copy(w_value, weights.at[2], local_sems.at[3]),
        pltpu.make_async_copy(w_gate, weights.at[3], local_sems.at[4]),
    ]
    for load in loads:
        load.start()
    exchanged = [
        remote(w_query, weights.at[0, :, mine], side_sems.at[0], side_sems.at[1], partner),
        remote(w_key, weights.at[1, :, mine], side_sems.at[2], side_sems.at[3], partner),
    ]
    for copy in exchanged:
        copy.start()
    for chip in range(CHIPS):
        columns = pl.ds(pl.multiple_of(chip * 2 * BLOCK + (1 - core) * BLOCK, BLOCK), BLOCK)
        remote(
            w_out.at[:, columns], other_out.at[chip], side_sems.at[4], side_sems.at[5], partner
        ).start()

    def wait_for(block, half):
        slot = held.at[block, rows_of(half)]
        remote(slot, slot, send_sems.at[0], recv_sems.at[block, half], partner).wait_recv()

    def arrive(da, db, half):
        block = place.at(da, db)
        wait_for(block, half)
        slot = held.at[block, rows_of(half)]
        if db == 0:
            if (da, half) == (-1, 0):
                send(slot, block, half, a_up)
            if (da, half) == (1, 1):
                send(slot, block, half, a_down)
            send(slot, block, half, b_up)
            send(slot, block, half, b_down)
        elif (db, half) == (-1, 0):
            send(slot, block, half, b_up)
        elif (db, half) == (1, 1):
            send(slot, block, half, b_down)
        send(slot, block, half, partner)

    def project(first, second, begin=False):
        def body(index, carry):
            which, half = lax.div(index, 2), lax.rem(index, 2)
            span = pl.ds(pl.multiple_of(half * sub, sub), sub)
            left = jnp.concatenate([held[first, span, :], held[second, span, :]], axis=1)
            right = jnp.concatenate(
                [
                    weights[which, pl.ds(pl.multiple_of(first * BLOCK, BLOCK), BLOCK), :],
                    weights[which, pl.ds(pl.multiple_of(second * BLOCK, BLOCK), BLOCK), :],
                ],
                axis=0,
            )
            part = jnp.dot(left, right, preferred_element_type=F32)
            if begin:
                total[which, span, :] = part
            else:
                total[which, span, :] += part
            return carry

        lax.fori_loop(0, 8, body, 0)

    def partner_pair(pair):
        blocks = [place.partner_at(*offset) for offset in pair]
        for block in blocks:
            for half in range(2):
                wait_for(block, half)
        project(*blocks)

    for stage, events in enumerate(ARRIVALS):
        for event in events:
            arrive(*event)
        if stage == 0:
            for load in loads:
                load.wait()
            for copy in exchanged:
                copy.wait()
            wait_for(partner, 0)
            wait_for(partner, 1)
            project(me, partner, begin=True)
        if stage in PAIRS:
            project(*[place.at(*offset) for offset in PAIRS[stage]])
        if stage - 1 in PAIRS:
            partner_pair(PAIRS[stage - 1])
    far, partner_far = place.at(2, 2), place.partner_at(2, 2)
    for half in range(2):
        wait_for(partner_far, half)
    project(far, partner_far)

    def finish(index, carry):
        span = pl.ds(pl.multiple_of(index * (rows // 8), rows // 8), rows // 8)
        query[span, :] = (total[0, span, :] * HEAD ** (-0.5)).astype(BF16)
        key_proj[span, :] = total[1, span, :].astype(BF16)
        value_proj[span, :] = total[2, span, :].astype(BF16)
        gate_proj[span, :] = total[3, span, :]
        return carry

    lax.fori_loop(0, 8, finish, 0)
    remote(other_out, other_out, side_sems.at[4], side_sems.at[5], partner).wait()
    for copy in sent:
        copy.wait_send()


def gather_and_project(tokens, w_query, w_key, w_value, w_gate, w_out):
    rows, features = tokens.shape[0], w_query.shape[0]
    half_flops = 2 * rows * features * 1024
    anywhere = pl.BlockSpec(memory_space=pl.ANY)
    inside = pl.BlockSpec(memory_space=pltpu.VMEM)
    return pl.pallas_call(
        gather_kernel,
        out_shape=(
            jax.ShapeDtypeStruct((rows, HEAD), BF16),
            jax.ShapeDtypeStruct((rows, HEAD), BF16),
            jax.ShapeDtypeStruct((rows, 256), BF16),
            jax.ShapeDtypeStruct((rows, 256), F32),
            jax.ShapeDtypeStruct((CHIPS, 256, BLOCK), BF16),
        ),
        in_specs=[anywhere] * 6,
        out_specs=(inside, inside, inside, inside, anywhere),
        scratch_shapes=[
            pltpu.VMEM((2 * CHIPS, rows, BLOCK), BF16),
            pltpu.VMEM((4, features, 256), BF16),
            pltpu.VMEM((4, rows, 256), F32),
            pltpu.SemaphoreType.DMA((64,)),
            pltpu.SemaphoreType.DMA((2 * CHIPS, 2)),
            pltpu.SemaphoreType.DMA((6,)),
            pltpu.SemaphoreType.DMA((5,)),
        ],
        compiler_params=pltpu.CompilerParams(
            collective_id=0, has_side_effects=True, vmem_limit_bytes=40 * 2**20
        ),
        cost_estimate=pl.CostEstimate(flops=half_flops, bytes_accessed=2**24, transcendentals=0),
        name="gather_project",
    )(tokens, w_query, w_key, w_value, w_gate, w_out)


def retention_kernel(
    query, key_proj, value_proj, gate_proj, decay, gain, state, new_state, retained, scale, stats
):
    head = lax.div(lax.axis_index("mp"), 2)
    rows = query.shape[0]
    sequences = rows // NEW
    rates = jnp.log(decay[...])
    lane = lax.broadcasted_iota(jnp.int32, rates.shape, 1)
    rate = jnp.sum(jnp.where(lane == head, rates, 0.0), axis=1, keepdims=True)
    rate = jnp.broadcast_to(rate, (rows, 128))
    to = lax.broadcasted_iota(jnp.int32, (rows, rows), 0)
    at = lax.broadcasted_iota(jnp.int32, (rows, rows), 1)
    same = lax.div(to, NEW) == lax.div(at, NEW)
    causal = jnp.logical_and(same, at <= to)
    cumul = jnp.dot(causal.astype(F32), rate, precision=HIGHEST, preferred_element_type=F32)
    final = jnp.dot(same.astype(F32), rate, precision=HIGHEST, preferred_element_type=F32)
    pick = (lax.broadcasted_iota(jnp.int32, (8, 128), 1) == 0).astype(F32)
    along = lax.dot_general(
        pick, cumul, (((1,), (1,)), ((), ())), precision=HIGHEST, preferred_element_type=F32
    )[:1, :]
    wide = jnp.concatenate([cumul] * (rows // 128), axis=1) if rows > 128 else cumul[:, :rows]
    gap = jnp.where(causal, wide - along, 0.0)
    factor = jnp.where(causal, jnp.exp(gap), 0.0)
    q, k, v = query[...], key_proj[...], value_proj[...]
    scores = lax.dot_general(q, k, (((1,), (1,)), ((), ())), preferred_element_type=F32)
    weights = (scores * factor).astype(BF16)
    in_block = jnp.dot(weights, v, preferred_element_type=F32)
    carry_scale = jnp.exp(final - cumul)
    decayed = (k.astype(F32) * jnp.concatenate([carry_scale] * 2, axis=1)).astype(BF16)
    from_scale = jnp.exp(cumul)
    from_scale = jnp.concatenate([from_scale] * 2, axis=1)
    final_scale = jnp.exp(final)
    final_scale = jnp.concatenate([final_scale] * 2, axis=1)
    for s in range(sequences):
        span = slice(s * NEW, (s + 1) * NEW)
        old = state[s]
        from_state = jnp.dot(q[span], old.astype(BF16), preferred_element_type=F32)
        retained[span, :] = from_scale[span] * from_state + in_block[span]
        fresh = lax.dot_general(
            decayed[span], v[span], (((0,), (0,)), ((), ())), preferred_element_type=F32
        )
        new_state[s] = final_scale[s * NEW : s * NEW + 1] * old + fresh
    values = retained[...]
    first = jnp.sum(values, axis=1, keepdims=True)
    second = jnp.sum(values * values, axis=1, keepdims=True)
    lanes = lax.broadcasted_iota(jnp.int32, (rows, 128), 1)
    stats[...] = jnp.where(lanes < 64, first, second)
    g = gate_proj[...]
    scale[...] = gain[...] * (g / (1.0 + jnp.exp(-g)))


def retention(query, key_proj, value_proj, gate_proj, decay, gain, state):
    rows = query.shape[0]
    tile = min(rows, 256)
    sequences = tile // NEW
    block = pl.BlockSpec((tile, 256), lambda i: (i, 0))
    return pl.pallas_call(
        retention_kernel,
        grid=(rows // tile,),
        out_shape=(
            jax.ShapeDtypeStruct(state.shape, F32),
            jax.ShapeDtypeStruct((rows, 256), F32),
            jax.ShapeDtypeStruct((rows, 256), F32),
            jax.ShapeDtypeStruct((rows, 128), F32),
        ),
        in_specs=[
            block,
            block,
            block,
            block,
            pl.BlockSpec((tile, decay.shape[1]), lambda i: (i, 0)),
            pl.BlockSpec((1, 256), lambda i: (0, 0)),
            pl.BlockSpec((sequences, 256, 256), lambda i: (i, 0, 0)),
        ],
        out_specs=(
            pl.BlockSpec((sequences, 256, 256), lambda i: (i, 0, 0)),
            block,
            block,
            pl.BlockSpec((tile, 128), lambda i: (i, 0)),
        ),
        compiler_params=pltpu.CompilerParams(vmem_limit_bytes=32 * 2**20),
        name="retention",
    )(query, key_proj, value_proj, gate_proj, decay, gain.reshape(1, -1), state)


ORDER = (2, 1, -1, 0)


def reduce_kernel(
    retained, scale, stats, w_out, other_out,
    layer_out,
    other_stats, gated, out_rows, s1, r1, s2, r2, column_sum,
    pair_sems, ss1, rs1, ss2, rs2, local_sems,
):
    place = Place()
    rows = retained.shape[0]
    sub = rows // 2
    core, partner = place.core, place.partner
    sent = []

    greet(place)
    exchange = remote(stats, other_stats, pair_sems.at[0], pair_sems.at[1], partner)
    exchange.start()
    loads = []
    own_rows = pl.ds(pl.multiple_of(core * 256, 256), 256)
    other_rows = pl.ds(pl.multiple_of((1 - core) * 256, 256), 256)
    for chip in range(CHIPS):
        columns = pl.ds(pl.multiple_of(chip * 2 * BLOCK + core * BLOCK, BLOCK), BLOCK)
        loads.append(
            pltpu.make_async_copy(w_out.at[:, columns], out_rows.at[chip, own_rows], local_sems.at[chip])
        )
    loads.append(pltpu.make_async_copy(other_out, out_rows.at[:, other_rows], local_sems.at[CHIPS]))
    for load in loads:
        load.start()
    exchange.wait_recv()
    tile = min(sub, 256)
    for half in range(2):
        def gate(index, carry):
            span = pl.ds(pl.multiple_of(half * sub + index * tile, tile), tile)
            both = stats[span, :] + other_stats[span, :]
            centre = both[:, :1] / VHEAD
            variance = both[:, 64:65] / VHEAD - centre * centre
            inverse = lax.rsqrt(variance + EPS)
            gated[core, span, :] = (
                (retained[span, :] - centre) * inverse * scale[span, :]
            ).astype(BF16)
            return carry

        lax.fori_loop(0, sub // tile, gate, 0)
        slot = gated.at[core, pl.ds(half * sub, sub)]
        copy = remote(slot, slot, pair_sems.at[2 + 2 * half], pair_sems.at[3 + 2 * half], partner)
        copy.start()
        sent.append(copy)
    for load in loads:
        load.wait()
    for half in range(2):
        slot = gated.at[1 - core, pl.ds(half * sub, sub)]
        remote(slot, slot, pair_sems.at[2 + 2 * half], pair_sems.at[3 + 2 * half], partner).wait_recv()

    def part(da, db, half):
        chip = place.chip(da, db)
        span = pl.ds(half * sub, sub)
        return jnp.dot(
            gated[0, span, :], out_rows[chip, :256, :], preferred_element_type=F32
        ) + jnp.dot(gated[1, span, :], out_rows[chip, 256:, :], preferred_element_type=F32)

    b_next = (place.at(0, 1), place.at(0, -1))
    a_next = (place.at(1, 0), place.at(-1, 0))

    def put1(way, kind, j, value):
        s1[way, kind, j] = value.astype(BF16)
        copy = remote(
            s1.at[way, kind, j], r1.at[way, kind, j], ss1.at[way, kind, j], rs1.at[way, kind, j], b_next[way]
        )
        copy.start()
        sent.append(copy)

    def got1(way, kind, j):
        remote(
            s1.at[way, kind, j], r1.at[way, kind, j], ss1.at[way, kind, j], rs1.at[way, kind, j], b_next[way]
        ).wait_recv()
        return r1[way, kind, j].astype(F32)

    def put2(way, kind, value):
        s2[way, kind] = value.astype(BF16)
        copy = remote(s2.at[way, kind], r2.at[way, kind], ss2.at[way, kind], rs2.at[way, kind], a_next[way])
        copy.start()
        sent.append(copy)

    def got2(way, kind):
        remote(
            s2.at[way, kind], r2.at[way, kind], ss2.at[way, kind], rs2.at[way, kind], a_next[way]
        ).wait_recv()
        return r2[way, kind].astype(F32)

    def far1(j):
        for way in range(2):
            put1(way, 0, j, part(ORDER[j], 2, way))

    def plain1(j):
        for way in range(2):
            put1(way, 1, j, part(ORDER[j], 1 - 2 * way, 1 - way))

    def sum1(j):
        for way in range(2):
            mine = part(ORDER[j], 1 - 2 * way, way)
            put1(way, 2, j, mine + got1(way, 0, j))

    def column(j, half):
        mine = part(ORDER[j], 0, half)
        return mine + got1(half, 2, j) + got1(1 - half, 1, j)

    far1(0)
    far1(1)
    plain1(0)
    sum1(0)
    far1(2)
    plain1(1)
    sum1(1)
    for half in range(2):
        put2(half, 0, column(0, half))
    far1(3)
    plain1(2)
    sum1(2)
    put2(0, 1, column(1, 1))
    mine = column(1, 0)
    put2(0, 2, mine + got2(0, 0))
    plain1(3)
    sum1(3)
    put2(1, 1, column(2, 0))
    mine = column(2, 1)
    put2(1, 2, mine + got2(1, 0))
    for half in range(2):
        column_sum[pl.ds(half * sub, sub), :] = column(3, half)
    for half in range(2):
        span = pl.ds(half * sub, sub)
        layer_out[span, :] = (column_sum[span, :] + got2(half, 2) + got2(1 - half, 1)).astype(BF16)
    exchange.wait_send()
    for copy in sent:
        copy.wait_send()


def project_and_reduce(retained, scale, stats, w_out, other_out):
    rows = retained.shape[0]
    sub = rows // 2
    anywhere = pl.BlockSpec(memory_space=pl.ANY)
    inside = pl.BlockSpec(memory_space=pltpu.VMEM)
    return pl.pallas_call(
        reduce_kernel,
        out_shape=jax.ShapeDtypeStruct((rows, BLOCK), BF16),
        in_specs=[inside, inside, inside, anywhere, anywhere],
        out_specs=inside,
        scratch_shapes=[
            pltpu.VMEM((rows, 128), F32),
            pltpu.VMEM((2, rows, 256), BF16),
            pltpu.VMEM((CHIPS, 512, BLOCK), BF16),
            pltpu.VMEM((2, 3, 4, sub, BLOCK), BF16),
            pltpu.VMEM((2, 3, 4, sub, BLOCK), BF16),
            pltpu.VMEM((2, 3, sub, BLOCK), BF16),
            pltpu.VMEM((2, 3, sub, BLOCK), BF16),
            pltpu.VMEM((rows, BLOCK), F32),
            pltpu.SemaphoreType.DMA((6,)),
            pltpu.SemaphoreType.DMA((2, 3, 4)),
            pltpu.SemaphoreType.DMA((2, 3, 4)),
            pltpu.SemaphoreType.DMA((2, 3)),
            pltpu.SemaphoreType.DMA((2, 3)),
            pltpu.SemaphoreType.DMA((CHIPS + 1,)),
        ],
        compiler_params=pltpu.CompilerParams(
            collective_id=1, has_side_effects=True, vmem_limit_bytes=32 * 2**20
        ),
        cost_estimate=pl.CostEstimate(flops=2 * rows * 512 * 2048, bytes_accessed=2**23, transcendentals=0),
        name="project_reduce",
    )(retained, scale, stats, w_out, other_out)


def per_device(tokens, decay, state, w_query, w_key, w_value, w_gate, w_out, norm_gain):
    query, key_proj, value_proj, gate_proj, other_out = gather_and_project(
        tokens, w_query, w_key, w_value, w_gate, w_out
    )
    new_state, retained, scale, stats = retention(
        query, key_proj, value_proj, gate_proj, decay, norm_gain, state
    )
    layer_out = project_and_reduce(retained, scale, stats, w_out, other_out)
    return layer_out, new_state


def solution(mesh):
    placed = (
        P("dp", "mp"),
        P("dp", None),
        P("dp", None, "mp"),
        P(None, "mp"),
        P(None, "mp"),
        P(None, "mp"),
        P(None, "mp"),
        P("mp", None),
        P("mp"),
    )
    return jax.shard_map(
        per_device,
        mesh=mesh,
        in_specs=placed,
        out_specs=(P("dp", "mp"), P("dp", None, "mp")),
        check_vma=False,
    )
```

```python
import functools

import jax
import jax.numpy as jnp
from jax import lax
from jax.experimental import pallas as pl
from jax.experimental.pallas import tpu as pltpu
from jax.sharding import PartitionSpec as P

HEAD = 256
VHEAD = 512
NEW = 32
EPS = 0.1
TILE = 512
UNROLL = 8
SIDE = 4
CHIPS = SIDE * SIDE
BLOCK = 128

MESH = pl.DeviceIdType.MESH
HIGHEST = lax.Precision.HIGHEST
BF16 = jnp.bfloat16
F32 = jnp.float32


class Place:
    def __init__(self):
        self.me = lax.axis_index("mp")
        self.core = lax.rem(self.me, 2)
        chip = lax.div(self.me, 2)
        y, x = lax.div(chip, SIDE), lax.rem(chip, SIDE)
        self.a = x * (1 - self.core) + y * self.core
        self.b = y * (1 - self.core) + x * self.core
        self.step_a = 1 + (SIDE - 1) * self.core
        self.step_b = SIDE - (SIDE - 1) * self.core
        self.partner = self.me + 1 - 2 * self.core

    def chip(self, da, db):
        a = lax.rem(self.a + (da + SIDE), SIDE)
        b = lax.rem(self.b + (db + SIDE), SIDE)
        return a * self.step_a + b * self.step_b

    def at(self, da, db):
        return self.chip(da, db) * 2 + self.core

    def partner_at(self, da, db):
        a = lax.rem(self.b + (da + SIDE), SIDE)
        b = lax.rem(self.a + (db + SIDE), SIDE)
        return (a * self.step_b + b * self.step_a) * 2 + 1 - self.core


def remote(src, dst, send_sem, recv_sem, device):
    return pltpu.make_async_remote_copy(
        src_ref=src,
        dst_ref=dst,
        send_sem=send_sem,
        recv_sem=recv_sem,
        device_id={"mp": device},
        device_id_type=MESH,
    )


def greet(place):
    barrier = pltpu.get_barrier_semaphore()
    others = (place.partner, place.at(1, 0), place.at(-1, 0), place.at(0, 1), place.at(0, -1))
    for other in others:
        pl.semaphore_signal(barrier, inc=1, device_id={"mp": other}, device_id_type=MESH)
    pl.semaphore_wait(barrier, len(others))


ARRIVALS = (
    ((-1, 0, 0), (1, 0, 0), (0, -1, 0), (0, 1, 0)),
    ((-1, 0, 1), (1, 0, 1)),
    ((0, -1, 1), (0, 1, 1)),
    ((-1, -1, 0), (-1, 1, 0), (1, -1, 0), (1, 1, 0), (2, 0, 0), (2, 0, 1), (0, 2, 0), (0, 2, 1)),
    ((-1, -1, 1), (-1, 1, 1)),
    ((1, -1, 1), (1, 1, 1)),
    ((2, -1, 0), (2, 1, 0), (2, -1, 1), (2, 1, 1)),
    ((-1, 2, 0), (-1, 2, 1), (1, 2, 0), (1, 2, 1)),
    ((2, 2, 0), (2, 2, 1)),
)
PAIRS = {
    1: ((-1, 0), (1, 0)),
    2: ((0, -1), (0, 1)),
    3: ((2, 0), (0, 2)),
    4: ((-1, -1), (-1, 1)),
    5: ((1, -1), (1, 1)),
    6: ((2, -1), (2, 1)),
    7: ((-1, 2), (1, 2)),
}


def gather_kernel(
    tokens, w_query, w_key, w_value, w_gate, w_out,
    query, key_proj, value_proj, gate_proj, other_out,
    held, weights, total, send_sems, recv_sems, side_sems, local_sems,
):
    place = Place()
    rows = tokens.shape[0]
    sub = rows // 2
    me, core, partner = place.me, place.core, place.partner
    sent = []

    def rows_of(half):
        return pl.ds(half * sub, sub)

    def send(src, block, half, device):
        copy = remote(
            src, held.at[block, rows_of(half)], send_sems.at[len(sent)], recv_sems.at[block, half], device
        )
        copy.start()
        sent.append(copy)

    greet(place)
    ring = (place.at(1, 0), place.at(-1, 0), place.at(0, 1), place.at(0, -1))
    a_up, a_down, b_up, b_down = ring
    for half in range(2):
        for device in ring + (partner,):
            send(tokens.at[rows_of(half)], me, half, device)
    mine = pl.ds(pl.multiple_of(core * BLOCK, BLOCK), BLOCK)
    loads = [
        pltpu.make_async_copy(tokens, held.at[me], local_sems.at[0]),
        pltpu.make_async_copy(w_query, weights.at[0, :, mine], local_sems.at[1]),
        pltpu.make_async_copy(w_key, weights.at[1, :, mine], local_sems.at[2]),
        pltpu.make_async_copy(w_value, weights.at[2], local_sems.at[3]),
        pltpu.make_async_copy(w_gate, weights.at[3], local_sems.at[4]),
    ]
    for load in loads:
        load.start()
    exchanged = [
        remote(w_query, weights.at[0, :, mine], side_sems.at[0], side_sems.at[1], partner),
        remote(w_key, weights.at[1, :, mine], side_sems.at[2], side_sems.at[3], partner),
    ]
    for copy in exchanged:
        copy.start()
    for chip in range(CHIPS):
        columns = pl.ds(pl.multiple_of(chip * 2 * BLOCK + (1 - core) * BLOCK, BLOCK), BLOCK)
        remote(
            w_out.at[:, columns], other_out.at[chip], side_sems.at[4], side_sems.at[5], partner
        ).start()

    def wait_for(block, half):
        slot = held.at[block, rows_of(half)]
        remote(slot, slot, send_sems.at[0], recv_sems.at[block, half], partner).wait_recv()

    def arrive(da, db, half):
        block = place.at(da, db)
        wait_for(block, half)
        slot = held.at[block, rows_of(half)]
        if db == 0:
            if (da, half) == (-1, 0):
                send(slot, block, half, a_up)
            if (da, half) == (1, 1):
                send(slot, block, half, a_down)
            send(slot, block, half, b_up)
            send(slot, block, half, b_down)
        elif (db, half) == (-1, 0):
            send(slot, block, half, b_up)
        elif (db, half) == (1, 1):
            send(slot, block, half, b_down)
        send(slot, block, half, partner)

    def project(*blocks, begin=False):
        starts = [pl.multiple_of(block * BLOCK, BLOCK) for block in blocks]

        def body(index, carry):
            which, tile = lax.div(index, rows // TILE), lax.rem(index, rows // TILE)
            span = pl.ds(pl.multiple_of(tile * TILE, TILE), TILE)
            left = jnp.concatenate([held[block, span, :] for block in blocks], axis=1)
            right = jnp.concatenate([weights[which, pl.ds(start, BLOCK), :] for start in starts], axis=0)
            part = jnp.dot(left, right, preferred_element_type=F32)
            if begin:
                total[which, span, :] = part
            else:
                total[which, span, :] += part
            return carry

        lax.fori_loop(0, 4 * (rows // TILE), body, 0, unroll=UNROLL)

    for stage, events in enumerate(ARRIVALS):
        for event in events:
            arrive(*event)
        if stage == 0:
            for load in loads:
                load.wait()
            for copy in exchanged:
                copy.wait()
            wait_for(partner, 0)
            wait_for(partner, 1)
            project(me, partner, begin=True)
        if stage - 1 in PAIRS:
            theirs = [place.partner_at(*offset) for offset in PAIRS[stage - 1]]
            for block in theirs:
                for half in range(2):
                    wait_for(block, half)
            project(*[place.at(*offset) for offset in PAIRS[stage - 1]], *theirs)
    far, partner_far = place.at(2, 2), place.partner_at(2, 2)
    for half in range(2):
        wait_for(partner_far, half)
    project(far, partner_far)

    def finish(index, carry):
        span = pl.ds(pl.multiple_of(index * (rows // 8), rows // 8), rows // 8)
        query[span, :] = (total[0, span, :] * HEAD ** (-0.5)).astype(BF16)
        key_proj[span, :] = total[1, span, :].astype(BF16)
        value_proj[span, :] = total[2, span, :].astype(BF16)
        gate_proj[span, :] = total[3, span, :]
        return carry

    lax.fori_loop(0, 8, finish, 0)
    remote(other_out, other_out, side_sems.at[4], side_sems.at[5], partner).wait()
    for copy in sent:
        copy.wait_send()


def gather_and_project(tokens, w_query, w_key, w_value, w_gate, w_out):
    rows, features = tokens.shape[0], w_query.shape[0]
    half_flops = 2 * rows * features * 1024
    anywhere = pl.BlockSpec(memory_space=pltpu.HBM)
    inside = pl.BlockSpec(memory_space=pltpu.VMEM)
    return pl.pallas_call(
        gather_kernel,
        out_shape=(
            jax.ShapeDtypeStruct((rows, HEAD), BF16),
            jax.ShapeDtypeStruct((rows, HEAD), BF16),
            jax.ShapeDtypeStruct((rows, 256), BF16),
            jax.ShapeDtypeStruct((rows, 256), F32),
            jax.ShapeDtypeStruct((CHIPS, 256, BLOCK), BF16),
        ),
        in_specs=[anywhere] * 6,
        out_specs=(inside, inside, inside, inside, anywhere),
        scratch_shapes=[
            pltpu.VMEM((2 * CHIPS, rows, BLOCK), BF16),
            pltpu.VMEM((4, features, 256), BF16),
            pltpu.VMEM((4, rows, 256), F32),
            pltpu.SemaphoreType.DMA((64,)),
            pltpu.SemaphoreType.DMA((2 * CHIPS, 2)),
            pltpu.SemaphoreType.DMA((6,)),
            pltpu.SemaphoreType.DMA((5,)),
        ],
        compiler_params=pltpu.CompilerParams(
            collective_id=0, has_side_effects=True, vmem_limit_bytes=40 * 2**20
        ),
        cost_estimate=pl.CostEstimate(flops=half_flops, bytes_accessed=2**24, transcendentals=0),
        name="gather_project",
    )(tokens, w_query, w_key, w_value, w_gate, w_out)


def retention_kernel(
    query, key_proj, value_proj, gate_proj, decay, gain, state, new_state, retained, scale, stats
):
    head = lax.div(lax.axis_index("mp"), 2)
    rows = query.shape[0]
    sequences = rows // NEW
    rates = jnp.log(decay[...])
    lane = lax.broadcasted_iota(jnp.int32, rates.shape, 1)
    rate = jnp.sum(jnp.where(lane == head, rates, 0.0), axis=1, keepdims=True)
    rate = jnp.broadcast_to(rate, (rows, 128))
    to = lax.broadcasted_iota(jnp.int32, (rows, rows), 0)
    at = lax.broadcasted_iota(jnp.int32, (rows, rows), 1)
    same = lax.div(to, NEW) == lax.div(at, NEW)
    causal = jnp.logical_and(same, at <= to)
    cumul = jnp.dot(causal.astype(F32), rate, precision=HIGHEST, preferred_element_type=F32)
    final = jnp.dot(same.astype(F32), rate, precision=HIGHEST, preferred_element_type=F32)
    pick = (lax.broadcasted_iota(jnp.int32, (8, 128), 1) == 0).astype(F32)
    along = lax.dot_general(
        pick, cumul, (((1,), (1,)), ((), ())), precision=HIGHEST, preferred_element_type=F32
    )[:1, :]
    wide = jnp.concatenate([cumul] * (rows // 128), axis=1) if rows > 128 else cumul[:, :rows]
    gap = jnp.where(causal, wide - along, 0.0)
    factor = jnp.where(causal, jnp.exp(gap), 0.0)
    q, k, v = query[...], key_proj[...], value_proj[...]
    scores = lax.dot_general(q, k, (((1,), (1,)), ((), ())), preferred_element_type=F32)
    weights = (scores * factor).astype(BF16)
    in_block = jnp.dot(weights, v, preferred_element_type=F32)
    carry_scale = jnp.exp(final - cumul)
    decayed = (k.astype(F32) * jnp.concatenate([carry_scale] * 2, axis=1)).astype(BF16)
    from_scale = jnp.exp(cumul)
    from_scale = jnp.concatenate([from_scale] * 2, axis=1)
    final_scale = jnp.exp(final)
    final_scale = jnp.concatenate([final_scale] * 2, axis=1)
    for s in range(sequences):
        span = slice(s * NEW, (s + 1) * NEW)
        old = state[s]
        from_state = jnp.dot(q[span], old.astype(BF16), preferred_element_type=F32)
        retained[span, :] = from_scale[span] * from_state + in_block[span]
        fresh = lax.dot_general(
            decayed[span], v[span], (((0,), (0,)), ((), ())), preferred_element_type=F32
        )
        new_state[s] = final_scale[s * NEW : s * NEW + 1] * old + fresh
    values = retained[...]
    first = jnp.sum(values, axis=1, keepdims=True)
    second = jnp.sum(values * values, axis=1, keepdims=True)
    lanes = lax.broadcasted_iota(jnp.int32, (rows, 128), 1)
    stats[...] = jnp.where(lanes < 64, first, second)
    g = gate_proj[...]
    scale[...] = gain[...] * (g / (1.0 + jnp.exp(-g)))


def retention(query, key_proj, value_proj, gate_proj, decay, gain, state):
    rows = query.shape[0]
    tile = min(rows, 256)
    sequences = tile // NEW
    block = pl.BlockSpec((tile, 256), lambda i: (i, 0))
    return pl.pallas_call(
        retention_kernel,
        grid=(rows // tile,),
        out_shape=(
            jax.ShapeDtypeStruct(state.shape, F32),
            jax.ShapeDtypeStruct((rows, 256), F32),
            jax.ShapeDtypeStruct((rows, 256), F32),
            jax.ShapeDtypeStruct((rows, 128), F32),
        ),
        in_specs=[
            block,
            block,
            block,
            block,
            pl.BlockSpec((tile, decay.shape[1]), lambda i: (i, 0)),
            pl.BlockSpec((1, 256), lambda i: (0, 0)),
            pl.BlockSpec((sequences, 256, 256), lambda i: (i, 0, 0)),
        ],
        out_specs=(
            pl.BlockSpec((sequences, 256, 256), lambda i: (i, 0, 0)),
            block,
            block,
            pl.BlockSpec((tile, 128), lambda i: (i, 0)),
        ),
        compiler_params=pltpu.CompilerParams(vmem_limit_bytes=60 * 2**20),
        name="retention",
    )(query, key_proj, value_proj, gate_proj, decay, gain.reshape(1, -1), state)


ORDER = (2, 1, -1, 0)


def reduce_kernel(
    retained, scale, stats, w_out, other_out,
    layer_out,
    other_stats, gated, out_rows, s1, r1, s2, r2, column_sum,
    pair_sems, ss1, rs1, ss2, rs2, local_sems,
):
    place = Place()
    rows = retained.shape[0]
    sub = rows // 2
    core, partner = place.core, place.partner
    sent = []

    greet(place)
    exchange = remote(stats, other_stats, pair_sems.at[0], pair_sems.at[1], partner)
    exchange.start()
    loads = []
    own_rows = pl.ds(pl.multiple_of(core * 256, 256), 256)
    other_rows = pl.ds(pl.multiple_of((1 - core) * 256, 256), 256)
    for chip in range(CHIPS):
        columns = pl.ds(pl.multiple_of(chip * 2 * BLOCK + core * BLOCK, BLOCK), BLOCK)
        loads.append(
            pltpu.make_async_copy(w_out.at[:, columns], out_rows.at[chip, own_rows], local_sems.at[chip])
        )
    loads.append(pltpu.make_async_copy(other_out, out_rows.at[:, other_rows], local_sems.at[CHIPS]))
    for load in loads:
        load.start()
    exchange.wait_recv()
    tile = min(sub, 256)
    for half in range(2):
        def gate(index, carry):
            span = pl.ds(pl.multiple_of(half * sub + index * tile, tile), tile)
            both = stats[span, :] + other_stats[span, :]
            centre = both[:, :1] / VHEAD
            variance = both[:, 64:65] / VHEAD - centre * centre
            inverse = lax.rsqrt(variance + EPS)
            gated[core, span, :] = (
                (retained[span, :] - centre) * inverse * scale[span, :]
            ).astype(BF16)
            return carry

        lax.fori_loop(0, sub // tile, gate, 0)
        slot = gated.at[core, pl.ds(half * sub, sub)]
        copy = remote(slot, slot, pair_sems.at[2 + 2 * half], pair_sems.at[3 + 2 * half], partner)
        copy.start()
        sent.append(copy)
    for load in loads:
        load.wait()
    for half in range(2):
        slot = gated.at[1 - core, pl.ds(half * sub, sub)]
        remote(slot, slot, pair_sems.at[2 + 2 * half], pair_sems.at[3 + 2 * half], partner).wait_recv()

    def part(da, db, half):
        chip = place.chip(da, db)
        span = pl.ds(half * sub, sub)
        return jnp.dot(
            gated[0, span, :], out_rows[chip, :256, :], preferred_element_type=F32
        ) + jnp.dot(gated[1, span, :], out_rows[chip, 256:, :], preferred_element_type=F32)

    b_next = (place.at(0, 1), place.at(0, -1))
    a_next = (place.at(1, 0), place.at(-1, 0))

    def put1(way, kind, j, value):
        s1[way, kind, j] = value.astype(BF16)
        copy = remote(
            s1.at[way, kind, j], r1.at[way, kind, j], ss1.at[way, kind, j], rs1.at[way, kind, j], b_next[way]
        )
        copy.start()
        sent.append(copy)

    def got1(way, kind, j):
        remote(
            s1.at[way, kind, j], r1.at[way, kind, j], ss1.at[way, kind, j], rs1.at[way, kind, j], b_next[way]
        ).wait_recv()
        return r1[way, kind, j].astype(F32)

    def put2(way, kind, value):
        s2[way, kind] = value.astype(BF16)
        copy = remote(s2.at[way, kind], r2.at[way, kind], ss2.at[way, kind], rs2.at[way, kind], a_next[way])
        copy.start()
        sent.append(copy)

    def got2(way, kind):
        remote(
            s2.at[way, kind], r2.at[way, kind], ss2.at[way, kind], rs2.at[way, kind], a_next[way]
        ).wait_recv()
        return r2[way, kind].astype(F32)

    def far1(j):
        for way in range(2):
            put1(way, 0, j, part(ORDER[j], 2, way))

    def plain1(j):
        for way in range(2):
            put1(way, 1, j, part(ORDER[j], 1 - 2 * way, 1 - way))

    def sum1(j):
        for way in range(2):
            mine = part(ORDER[j], 1 - 2 * way, way)
            put1(way, 2, j, mine + got1(way, 0, j))

    def column(j, half):
        mine = part(ORDER[j], 0, half)
        return mine + got1(half, 2, j) + got1(1 - half, 1, j)

    far1(0)
    far1(1)
    plain1(0)
    sum1(0)
    far1(2)
    plain1(1)
    sum1(1)
    for half in range(2):
        put2(half, 0, column(0, half))
    far1(3)
    plain1(2)
    sum1(2)
    put2(0, 1, column(1, 1))
    mine = column(1, 0)
    put2(0, 2, mine + got2(0, 0))
    plain1(3)
    sum1(3)
    put2(1, 1, column(2, 0))
    mine = column(2, 1)
    put2(1, 2, mine + got2(1, 0))
    for half in range(2):
        column_sum[pl.ds(half * sub, sub), :] = column(3, half)
    for half in range(2):
        span = pl.ds(half * sub, sub)
        layer_out[span, :] = (column_sum[span, :] + got2(half, 2) + got2(1 - half, 1)).astype(BF16)
    exchange.wait_send()
    for copy in sent:
        copy.wait_send()


def project_and_reduce(retained, scale, stats, w_out, other_out):
    rows = retained.shape[0]
    sub = rows // 2
    anywhere = pl.BlockSpec(memory_space=pltpu.HBM)
    inside = pl.BlockSpec(memory_space=pltpu.VMEM)
    return pl.pallas_call(
        reduce_kernel,
        out_shape=jax.ShapeDtypeStruct((rows, BLOCK), BF16),
        in_specs=[inside, inside, inside, anywhere, anywhere],
        out_specs=inside,
        scratch_shapes=[
            pltpu.VMEM((rows, 128), F32),
            pltpu.VMEM((2, rows, 256), BF16),
            pltpu.VMEM((CHIPS, 512, BLOCK), BF16),
            pltpu.VMEM((2, 3, 4, sub, BLOCK), BF16),
            pltpu.VMEM((2, 3, 4, sub, BLOCK), BF16),
            pltpu.VMEM((2, 3, sub, BLOCK), BF16),
            pltpu.VMEM((2, 3, sub, BLOCK), BF16),
            pltpu.VMEM((rows, BLOCK), F32),
            pltpu.SemaphoreType.DMA((6,)),
            pltpu.SemaphoreType.DMA((2, 3, 4)),
            pltpu.SemaphoreType.DMA((2, 3, 4)),
            pltpu.SemaphoreType.DMA((2, 3)),
            pltpu.SemaphoreType.DMA((2, 3)),
            pltpu.SemaphoreType.DMA((CHIPS + 1,)),
        ],
        compiler_params=pltpu.CompilerParams(
            collective_id=1, has_side_effects=True, vmem_limit_bytes=32 * 2**20
        ),
        cost_estimate=pl.CostEstimate(flops=2 * rows * 512 * 2048, bytes_accessed=2**23, transcendentals=0),
        name="project_reduce",
    )(retained, scale, stats, w_out, other_out)


def per_device(tokens, decay, state, w_query, w_key, w_value, w_gate, w_out, norm_gain):
    query, key_proj, value_proj, gate_proj, other_out = gather_and_project(
        tokens, w_query, w_key, w_value, w_gate, w_out
    )
    new_state, retained, scale, stats = retention(
        query, key_proj, value_proj, gate_proj, decay, norm_gain, state
    )
    layer_out = project_and_reduce(retained, scale, stats, w_out, other_out)
    return layer_out, new_state


def solution(mesh):
    placed = (
        P("dp", "mp"),
        P("dp", None),
        P("dp", None, "mp"),
        P(None, "mp"),
        P(None, "mp"),
        P(None, "mp"),
        P(None, "mp"),
        P("mp", None),
        P("mp"),
    )
    return jax.shard_map(
        per_device,
        mesh=mesh,
        in_specs=placed,
        out_specs=(P("dp", "mp"), P("dp", None, "mp")),
        check_vma=False,
    )
```

```python
import functools

import jax
import jax.numpy as jnp
from jax import lax
from jax.experimental import pallas as pl
from jax.experimental.pallas import tpu as pltpu
from jax.sharding import PartitionSpec as P

HEAD = 256
VHEAD = 512
NEW = 32
EPS = 0.1
CHUNKS = 2
STEPS = 8
VMEM_LIMIT = 62 * 2**20
SIDE = 4
CHIPS = SIDE * SIDE
BLOCK = 128

MESH = pl.DeviceIdType.MESH
HIGHEST = lax.Precision.HIGHEST
BF16 = jnp.bfloat16
F32 = jnp.float32


class Place:
    def __init__(self):
        self.me = lax.axis_index("mp")
        self.core = lax.rem(self.me, 2)
        chip = lax.div(self.me, 2)
        y, x = lax.div(chip, SIDE), lax.rem(chip, SIDE)
        self.a = x * (1 - self.core) + y * self.core
        self.b = y * (1 - self.core) + x * self.core
        self.step_a = 1 + (SIDE - 1) * self.core
        self.step_b = SIDE - (SIDE - 1) * self.core
        self.partner = self.me + 1 - 2 * self.core

    def chip(self, da, db):
        a = lax.rem(self.a + (da + SIDE), SIDE)
        b = lax.rem(self.b + (db + SIDE), SIDE)
        return a * self.step_a + b * self.step_b

    def at(self, da, db):
        return self.chip(da, db) * 2 + self.core

    def partner_at(self, da, db):
        a = lax.rem(self.b + (da + SIDE), SIDE)
        b = lax.rem(self.a + (db + SIDE), SIDE)
        return (a * self.step_b + b * self.step_a) * 2 + 1 - self.core


def remote(src, dst, send_sem, recv_sem, device):
    return pltpu.make_async_remote_copy(
        src_ref=src,
        dst_ref=dst,
        send_sem=send_sem,
        recv_sem=recv_sem,
        device_id={"mp": device},
        device_id_type=MESH,
    )


def greet(place):
    barrier = pltpu.get_barrier_semaphore()
    others = (place.partner, place.at(1, 0), place.at(-1, 0), place.at(0, 1), place.at(0, -1))
    for other in others:
        pl.semaphore_signal(barrier, inc=1, device_id={"mp": other}, device_id_type=MESH)
    pl.semaphore_wait(barrier, len(others))


ARRIVALS = (
    ((-1, 0, 0), (1, 0, 0), (0, -1, 0), (0, 1, 0)),
    ((-1, 0, 1), (1, 0, 1)),
    ((0, -1, 1), (0, 1, 1)),
    ((-1, -1, 0), (-1, 1, 0), (1, -1, 0), (1, 1, 0), (2, 0, 0), (2, 0, 1), (0, 2, 0), (0, 2, 1)),
    ((-1, -1, 1), (-1, 1, 1)),
    ((1, -1, 1), (1, 1, 1)),
    ((2, -1, 0), (2, 1, 0), (2, -1, 1), (2, 1, 1)),
    ((-1, 2, 0), (-1, 2, 1), (1, 2, 0), (1, 2, 1)),
    ((2, 2, 0), (2, 2, 1)),
)
PAIRS = {
    1: ((-1, 0), (1, 0)),
    2: ((0, -1), (0, 1)),
    3: ((2, 0), (0, 2)),
    4: ((-1, -1), (-1, 1)),
    5: ((1, -1), (1, 1)),
    6: ((2, -1), (2, 1)),
    7: ((-1, 2), (1, 2)),
}


ORDER = (2, 1, -1, 0)
GROUP = 256
PAIR_NT = (((1,), (1,)), ((), ()))
PAIR_TN = (((0,), (0,)), ((), ()))


def kernel(
    tokens, decay, gain, state, w_query, w_key, w_value, w_gate, w_out,
    layer_out, decayed_out, value_out, scale_out,
    held, old_state, decayed, values, scales, weights, total, out_rows, cumul, final, along,
    retained, stats, other_stats, gated, own1, near1, s1, r1, s2, r2, own2,
    send_sems, recv_sems, side_sems, load_sems, stat_sems, gate_sems, ss1, rs1, ss2, rs2, out_sems,
):
    place = Place()
    rows = tokens.shape[0]
    chunk = rows // CHUNKS
    sub = chunk // 2
    group = min(GROUP, chunk)
    me, core, partner = place.me, place.core, place.partner
    a_next = (place.at(1, 0), place.at(-1, 0))
    b_next = (place.at(0, 1), place.at(0, -1))
    sent, kept_copies = [], []
    counts = [0]

    greet(place)


    def rows_of(c, half):
        return pl.ds(c * chunk + half * sub, sub)

    def send(src, block, c, half, device):
        copy = remote(
            src, held.at[block, rows_of(c, half)],
            send_sems.at[counts[0]], recv_sems.at[c, block, half], device,
        )
        counts[0] += 1
        copy.start()
        sent.append(copy)

    def own(c, devices):
        for half in range(2):
            for device in devices:
                send(tokens.at[rows_of(c, half)], me, c, half, device)

    def wait_for(block, c, half):
        slot = held.at[block, rows_of(c, half)]
        remote(slot, slot, send_sems.at[0], recv_sems.at[c, block, half], partner).wait_recv()

    def arrive(c, da, db, half):
        block = place.at(da, db)
        wait_for(block, c, half)
        slot = held.at[block, rows_of(c, half)]
        if db == 0:
            if (da, half) == (-1, 0):
                send(slot, block, c, half, a_next[0])
            if (da, half) == (1, 1):
                send(slot, block, c, half, a_next[1])
            send(slot, block, c, half, b_next[0])
            send(slot, block, c, half, b_next[1])
        elif (db, half) == (-1, 0):
            send(slot, block, c, half, b_next[0])
        elif (db, half) == (1, 1):
            send(slot, block, c, half, b_next[1])
        send(slot, block, c, half, partner)

    def arrivals(c, stage):
        for event in ARRIVALS[stage]:
            arrive(c, *event)

    def project(c, step):
        if step == 0:
            theirs, blocks = [partner], [me, partner]
        elif step in PAIRS:
            theirs = [place.partner_at(*offset) for offset in PAIRS[step]]
            blocks = [place.at(*offset) for offset in PAIRS[step]] + theirs
        else:
            theirs = [place.partner_at(2, 2)]
            blocks = [place.at(2, 2)] + theirs
        for block in theirs:
            for half in range(2):
                wait_for(block, c, half)
        starts = [pl.multiple_of(block * BLOCK, BLOCK) for block in blocks]
        span = pl.ds(c * chunk, chunk)

        def body(which, carry):
            left = jnp.concatenate([held[block, span, :] for block in blocks], axis=1)
            right = jnp.concatenate([weights[which, pl.ds(start, BLOCK), :] for start in starts], axis=0)
            part = jnp.dot(left, right, preferred_element_type=F32)
            if step == 0:
                total[which, span, :] = part
            else:
                total[which, span, :] += part
            return carry

        lax.fori_loop(0, 4, body, 0, unroll=4)


    def decays():
        head = lax.div(me, 2)
        rates = jnp.log(decay[...])
        lane = lax.broadcasted_iota(jnp.int32, rates.shape, 0)
        rate = jnp.sum(jnp.where(lane == head, rates, 0.0), axis=0, keepdims=True)
        to = lax.broadcasted_iota(jnp.int32, (group, group), 0)
        at = lax.broadcasted_iota(jnp.int32, (group, group), 1)
        same = lax.div(to, NEW) == lax.div(at, NEW)
        causal = jnp.logical_and(same, at <= to).astype(F32)
        for g in range(rows // group):
            mine = rate[:, g * group : (g + 1) * group]
            mine = jnp.broadcast_to(mine, (128, group))
            span = slice(g * group, (g + 1) * group)
            cumul[span, :] = lax.dot_general(
                causal, mine, PAIR_NT, precision=HIGHEST, preferred_element_type=F32
            )
            final[span, :] = lax.dot_general(
                same.astype(F32), mine, PAIR_NT, precision=HIGHEST, preferred_element_type=F32
            )
            along[g] = lax.dot_general(
                mine[:8], causal, PAIR_NT, precision=HIGHEST, preferred_element_type=F32
            )

    def retain(g):
        span = pl.ds(g * group, group)
        query = (total[0, span, :] * HEAD ** (-0.5)).astype(BF16)
        key = total[1, span, :].astype(BF16)
        value = total[2, span, :].astype(BF16)
        to = lax.broadcasted_iota(jnp.int32, (group, group), 0)
        at = lax.broadcasted_iota(jnp.int32, (group, group), 1)
        causal = jnp.logical_and(lax.div(to, NEW) == lax.div(at, NEW), at <= to)
        c = cumul[span, :]
        wide = jnp.concatenate([c] * (group // 128), axis=1) if group > 128 else c[:, :group]
        gap = jnp.where(causal, wide - along[g, :1, :], 0.0)
        factor = jnp.where(causal, jnp.exp(gap), 0.0)
        scores = lax.dot_general(query, key, PAIR_NT, preferred_element_type=F32)
        weight = (scores * factor).astype(BF16)
        in_block = jnp.dot(weight, value, preferred_element_type=F32)
        last = final[span, :]
        carry_scale = jnp.exp(last - c)
        faded = (key.astype(F32) * jnp.concatenate([carry_scale] * 2, axis=1)).astype(BF16)
        from_scale = jnp.exp(c)
        from_scale = jnp.concatenate([from_scale] * 2, axis=1)
        last_scale = jnp.exp(last)
        last_scale = jnp.concatenate([last_scale] * 2, axis=1)
        parts = []
        for s in range(group // NEW):
            part = slice(s * NEW, (s + 1) * NEW)
            old = old_state[g * (group // NEW) + s]
            from_state = jnp.dot(query[part], old.astype(BF16), preferred_element_type=F32)
            parts.append(from_scale[part] * from_state + in_block[part])
            scales[pl.ds((g * (group // NEW) + s) * 8, 8), :] = last_scale[s * NEW : s * NEW + 8]
        kept = jnp.concatenate(parts, axis=0)
        retained[span, :] = kept
        decayed[span, :] = faded
        values[span, :] = value
        first = jnp.sum(kept, axis=1, keepdims=True)
        second = jnp.sum(kept * kept, axis=1, keepdims=True)
        lanes = lax.broadcasted_iota(jnp.int32, (group, 128), 1)
        stats[span, :] = jnp.where(lanes < 64, first, second)

    def keep(c):
        wide, narrow = pl.ds(c * chunk, chunk), pl.ds(c * (chunk // 4), chunk // 4)
        for i, (src, dst, span) in enumerate(
            ((decayed, decayed_out, wide), (values, value_out, wide), (scales, scale_out, narrow))
        ):
            copy = pltpu.make_async_copy(src.at[span], dst.at[span], out_sems.at[c, i])
            copy.start()
            kept_copies.append(copy)

    def stat_copy(c):
        span = pl.ds(c * chunk, chunk)
        return remote(stats.at[span], other_stats.at[span], stat_sems.at[c, 0], stat_sems.at[c, 1], partner)

    def share_stats(c):
        copy = stat_copy(c)
        copy.start()
        sent.append(copy)

    def gate_copy(c, owner):
        slot = gated.at[owner, pl.ds(c * chunk, chunk)]
        return remote(slot, slot, gate_sems.at[c, 0], gate_sems.at[c, 1], partner)

    def gate(c):
        stat_copy(c).wait_recv()
        tile = min(chunk, 128)

        def body(index, carry):
            span = pl.ds(pl.multiple_of(c * chunk + index * tile, tile), tile)
            both = stats[span, :] + other_stats[span, :]
            centre = both[:, :1] / VHEAD
            variance = both[:, 64:65] / VHEAD - centre * centre
            normed = (retained[span, :] - centre) * lax.rsqrt(variance + EPS)
            g = total[3, span, :]
            gated[core, span, :] = (normed * gain[...] * (g / (1.0 + jnp.exp(-g)))).astype(BF16)
            return carry

        lax.fori_loop(0, chunk // tile, body, 0, unroll=2)
        copy = gate_copy(c, core)
        copy.start()
        sent.append(copy)


    def products(c, j, first, second):
        span = pl.ds(c * chunk, chunk)
        left = jnp.concatenate([gated[0, span, :], gated[1, span, :]], axis=1)
        right = jnp.concatenate(
            [out_rows[place.chip(ORDER[j], first)], out_rows[place.chip(ORDER[j], second)]], axis=1
        )
        return jnp.dot(left, right, preferred_element_type=F32)

    def copy1(c, way, kind, j):
        at = (c, way, kind, j)
        return remote(s1.at[at], r1.at[at], ss1.at[at], rs1.at[at], b_next[way])

    def copy2(c, way, kind):
        at = (c, way, kind)
        return remote(s2.at[at], r2.at[at], ss2.at[at], rs2.at[at], a_next[way])

    def put1(c, way, kind, j, value):
        s1[c, way, kind, j] = value.astype(BF16)
        copy = copy1(c, way, kind, j)
        copy.start()
        sent.append(copy)

    def got1(c, way, kind, j):
        copy1(c, way, kind, j).wait_recv()
        return r1[c, way, kind, j].astype(F32)

    def put2(c, way, kind, value):
        s2[c, way, kind] = value.astype(BF16)
        copy = copy2(c, way, kind)
        copy.start()
        sent.append(copy)

    def got2(c, way, kind):
        copy2(c, way, kind).wait_recv()
        return r2[c, way, kind].astype(F32)

    def far(c, j):
        both = products(c, j, 2, 0)
        put1(c, 0, 0, j, both[:sub, :BLOCK])
        put1(c, 1, 0, j, both[sub:, :BLOCK])
        own1[c, j] = both[:, BLOCK:]

    def plain(c, j):
        both = products(c, j, 1, -1)
        put1(c, 0, 1, j, both[sub:, :BLOCK])
        put1(c, 1, 1, j, both[:sub, BLOCK:])
        near1[c, 0, j] = both[:sub, :BLOCK]
        near1[c, 1, j] = both[sub:, BLOCK:]

    def passing(c, j, way):
        put1(c, way, 2, j, near1[c, way, j] + got1(c, way, 0, j))

    def column(c, j, half):
        return own1[c, j, pl.ds(half * sub, sub), :] + got1(c, half, 2, j) + got1(c, 1 - half, 1, j)

    def row_far(c, way):
        put2(c, way, 0, column(c, 0, way))

    def row_plain(c, way):
        put2(c, way, 1, column(c, 1 + way, 1 - way))

    def row_passing(c, way):
        put2(c, way, 2, column(c, 1 + way, way) + got2(c, way, 0))

    def row_own(c, half):
        own2[rows_of(c, half), :] = column(c, 3, half)

    def finish(c, half):
        span = rows_of(c, half)
        layer_out[span, :] = (own2[span, :] + got2(c, half, 2) + got2(c, 1 - half, 1)).astype(BF16)


    mine = pl.ds(pl.multiple_of(core * BLOCK, BLOCK), BLOCK)
    own_rows = pl.ds(pl.multiple_of(core * 256, 256), 256)
    other_rows = pl.ds(pl.multiple_of((1 - core) * 256, 256), 256)
    loads = [
        pltpu.make_async_copy(tokens, held.at[me], load_sems.at[0]),
        pltpu.make_async_copy(w_query, weights.at[0, :, mine], load_sems.at[1]),
        pltpu.make_async_copy(w_key, weights.at[1, :, mine], load_sems.at[2]),
        pltpu.make_async_copy(w_value, weights.at[2], load_sems.at[3]),
        pltpu.make_async_copy(w_gate, weights.at[3], load_sems.at[4]),
    ]
    exchanged = [
        remote(w_query, weights.at[0, :, mine], side_sems.at[0], side_sems.at[1], partner),
        remote(w_key, weights.at[1, :, mine], side_sems.at[2], side_sems.at[3], partner),
    ]
    state_load = pltpu.make_async_copy(state, old_state, load_sems.at[5])
    out_loads = []
    out_sent = remote(out_rows.at[:, other_rows], out_rows.at[:, other_rows], side_sems.at[4], side_sems.at[5], partner)

    def start_out():
        for chip in range(CHIPS):
            columns = pl.ds(pl.multiple_of(chip * 2 * BLOCK + core * BLOCK, BLOCK), BLOCK)
            load = pltpu.make_async_copy(
                w_out.at[:, columns], out_rows.at[chip, own_rows], load_sems.at[6 + chip]
            )
            load.start()
            out_loads.append(load)
        for chip in range(CHIPS):
            columns = pl.ds(pl.multiple_of(chip * 2 * BLOCK + (1 - core) * BLOCK, BLOCK), BLOCK)
            remote(
                w_out.at[:, columns], out_rows.at[chip, own_rows], side_sems.at[4], side_sems.at[5], partner
            ).start()

    def wait_out():
        for load in out_loads:
            load.wait()
        out_sent.wait()

    ring = a_next + b_next
    own(0, a_next)
    own(0, b_next)
    own(0, (partner,))
    for load in loads:
        load.start()
    for copy in exchanged:
        copy.start()
    state_load.start()
    own(1, a_next)
    own(1, b_next)
    own(1, (partner,))
    decays()
    arrive(0, -1, 0, 0)
    arrive(0, 1, 0, 0)
    arrive(0, 0, -1, 0)
    arrive(0, 0, 1, 0)
    arrive(0, -1, 0, 1)
    arrive(0, 1, 0, 1)
    arrive(0, 0, 1, 1)
    arrive(0, 0, -1, 1)
    for load in loads:
        load.wait()
    for copy in exchanged:
        copy.wait()
    project(0, 0)
    project(1, 0)
    arrive(1, -1, 0, 0)
    arrive(1, 1, 0, 0)
    arrive(1, 0, -1, 0)
    arrive(1, 0, 1, 0)
    project(0, 1)
    project(0, 2)
    start_out()
    arrive(1, -1, 0, 1)
    arrive(1, 1, 0, 1)
    arrive(1, 0, 1, 1)
    arrive(1, 0, -1, 1)
    arrive(0, -1, 1, 0)
    arrive(0, 2, 0, 0)
    arrive(0, -1, -1, 0)
    arrive(0, 2, 0, 1)
    arrive(0, 1, 1, 0)
    arrive(0, 1, -1, 0)
    arrive(0, -1, 1, 1)
    arrive(1, 2, 0, 0)
    arrive(0, 0, 2, 0)
    arrive(0, 1, 1, 1)
    arrive(0, -1, -1, 1)
    arrive(1, 2, 0, 1)
    project(1, 1)
    arrive(0, 0, 2, 1)
    arrive(0, 1, -1, 1)
    project(1, 2)
    wait_out()
    arrive(1, -1, -1, 0)
    arrive(1, -1, 1, 0)
    project(0, 4)
    arrive(1, 1, -1, 0)
    arrive(1, 1, 1, 0)
    project(0, 3)
    arrive(1, -1, 1, 1)
    arrive(1, 0, 2, 0)
    project(0, 5)
    arrive(1, 1, 1, 1)
    arrive(1, -1, -1, 1)
    arrive(1, 0, 2, 1)
    arrive(1, 1, -1, 1)
    project(1, 4)
    arrive(0, 2, -1, 0)
    arrive(0, 2, 1, 0)
    project(1, 3)
    arrive(0, 2, 1, 1)
    arrive(0, -1, 2, 0)
    project(1, 5)
    arrive(0, -1, 2, 1)
    arrive(0, 2, -1, 1)
    arrive(0, 1, 2, 0)
    arrive(1, 2, 1, 0)
    arrive(1, 2, -1, 0)
    arrive(0, 1, 2, 1)
    project(0, 6)
    arrive(1, 2, 1, 1)
    arrive(1, 2, -1, 1)
    project(0, 7)
    arrive(1, -1, 2, 0)
    arrive(1, -1, 2, 1)
    arrive(1, 1, 2, 0)
    arrive(1, 1, 2, 1)
    project(1, 6)
    arrive(0, 2, 2, 0)
    arrive(0, 2, 2, 1)
    project(1, 7)
    arrive(1, 2, 2, 0)
    arrive(1, 2, 2, 1)
    project(0, 8)
    state_load.wait()
    retain(0)
    retain(1)
    share_stats(0)
    project(1, 8)
    retain(2)
    retain(3)
    share_stats(1)
    gate(0)
    keep(0)
    keep(1)
    gate(1)
    gate_copy(0, 1 - core).wait_recv()
    plain(0, 0)
    plain(0, 1)
    plain(0, 2)
    far(0, 0)
    gate_copy(1, 1 - core).wait_recv()
    plain(1, 0)
    plain(1, 1)
    plain(1, 2)
    far(1, 0)
    plain(0, 3)
    plain(1, 3)
    far(0, 1)
    far(1, 1)
    passing(0, 0, 0)
    passing(0, 0, 1)
    far(0, 2)
    far(1, 2)
    far(0, 3)
    far(1, 3)
    passing(1, 0, 0)
    passing(1, 0, 1)
    passing(0, 1, 0)
    passing(0, 1, 1)
    passing(1, 1, 0)
    passing(1, 1, 1)
    row_far(0, 0)
    row_far(0, 1)
    passing(0, 2, 0)
    passing(0, 2, 1)
    passing(1, 2, 0)
    passing(1, 2, 1)
    passing(0, 3, 0)
    passing(0, 3, 1)
    passing(1, 3, 0)
    passing(1, 3, 1)
    row_far(1, 0)
    row_far(1, 1)
    row_passing(0, 0)
    row_plain(0, 0)
    row_plain(1, 0)
    row_passing(0, 1)
    row_plain(0, 1)
    row_passing(1, 0)
    row_passing(1, 1)
    row_plain(1, 1)
    row_own(0, 1)
    row_own(0, 0)
    row_own(1, 1)
    finish(0, 1)
    finish(0, 0)
    row_own(1, 0)
    finish(1, 1)
    finish(1, 0)

    for copy in sent:
        copy.wait_send()
    for copy in kept_copies:
        copy.wait()


def update_kernel(state, decayed, values, scales, new_state, block, keys, held, scale, read_sems, write_sems, in_sems):
    count = state.shape[0]
    step = count // STEPS
    reads, writes = [], []
    inputs = [
        pltpu.make_async_copy(decayed, keys, in_sems.at[0]),
        pltpu.make_async_copy(values, held, in_sems.at[1]),
        pltpu.make_async_copy(scales, scale, in_sems.at[2]),
    ]
    for i in range(STEPS):
        span = pl.ds(i * step, step)
        reads.append(pltpu.make_async_copy(state.at[span], block.at[span], read_sems.at[i]))
        writes.append(pltpu.make_async_copy(block.at[span], new_state.at[span], write_sems.at[i]))
        reads[i].start()
        if i == 0:
            for copy in inputs:
                copy.start()
    for copy in inputs:
        copy.wait()
    for i in range(STEPS):
        reads[i].wait()
        for s in range(i * step, (i + 1) * step):
            part = slice(s * NEW, (s + 1) * NEW)
            fresh = lax.dot_general(keys[part, :], held[part, :], PAIR_TN, preferred_element_type=F32)
            block[s] = scale[s * 8 : s * 8 + 1, :] * block[s] + fresh
        writes[i].start()
    for write in writes:
        write.wait()


def update_state(state, decayed, values, scales):
    outside = pl.BlockSpec(memory_space=pltpu.HBM)
    return pl.pallas_call(
        update_kernel,
        out_shape=jax.ShapeDtypeStruct(state.shape, F32),
        in_specs=[outside] * 4,
        out_specs=outside,
        scratch_shapes=[
            pltpu.VMEM(state.shape, F32),
            pltpu.VMEM(decayed.shape, BF16),
            pltpu.VMEM(values.shape, BF16),
            pltpu.VMEM(scales.shape, F32),
            pltpu.SemaphoreType.DMA((STEPS,)),
            pltpu.SemaphoreType.DMA((STEPS,)),
            pltpu.SemaphoreType.DMA((3,)),
        ],
        compiler_params=pltpu.CompilerParams(vmem_limit_bytes=VMEM_LIMIT),
        name="update_state",
    )(state, decayed, values, scales)


def per_device(tokens, decay, state, w_query, w_key, w_value, w_gate, w_out, norm_gain):
    rows, features = tokens.shape[0], w_query.shape[0]
    chunk = rows // CHUNKS
    sub = chunk // 2
    group = min(GROUP, chunk)
    outside = pl.BlockSpec(memory_space=pltpu.HBM)
    inside = pl.BlockSpec(memory_space=pltpu.VMEM)
    layer_out, decayed, values, scales = pl.pallas_call(
        kernel,
        out_shape=(
            jax.ShapeDtypeStruct((rows, BLOCK), BF16),
            jax.ShapeDtypeStruct((rows, 256), BF16),
            jax.ShapeDtypeStruct((rows, 256), BF16),
            jax.ShapeDtypeStruct((rows // 4, 256), F32),
        ),
        in_specs=[outside, inside, inside] + [outside] * 6,
        out_specs=(inside, outside, outside, outside),
        scratch_shapes=[
            pltpu.VMEM((2 * CHIPS, rows, BLOCK), BF16),
            pltpu.VMEM(state.shape, F32),
            pltpu.VMEM((rows, 256), BF16),
            pltpu.VMEM((rows, 256), BF16),
            pltpu.VMEM((rows // 4, 256), F32),
            pltpu.VMEM((4, features, 256), BF16),
            pltpu.VMEM((4, rows, 256), F32),
            pltpu.VMEM((CHIPS, 512, BLOCK), BF16),
            pltpu.VMEM((rows, 128), F32),
            pltpu.VMEM((rows, 128), F32),
            pltpu.VMEM((rows // group, 8, group), F32),
            pltpu.VMEM((rows, 256), F32),
            pltpu.VMEM((rows, 128), F32),
            pltpu.VMEM((rows, 128), F32),
            pltpu.VMEM((2, rows, 256), BF16),
            pltpu.VMEM((CHUNKS, 4, chunk, BLOCK), F32),
            pltpu.VMEM((CHUNKS, 2, 4, sub, BLOCK), F32),
            pltpu.VMEM((CHUNKS, 2, 3, 4, sub, BLOCK), BF16),
            pltpu.VMEM((CHUNKS, 2, 3, 4, sub, BLOCK), BF16),
            pltpu.VMEM((CHUNKS, 2, 3, sub, BLOCK), BF16),
            pltpu.VMEM((CHUNKS, 2, 3, sub, BLOCK), BF16),
            pltpu.VMEM((rows, BLOCK), F32),
            pltpu.SemaphoreType.DMA((CHUNKS * 64,)),
            pltpu.SemaphoreType.DMA((CHUNKS, 2 * CHIPS, 2)),
            pltpu.SemaphoreType.DMA((6,)),
            pltpu.SemaphoreType.DMA((6 + CHIPS,)),
            pltpu.SemaphoreType.DMA((CHUNKS, 2)),
            pltpu.SemaphoreType.DMA((CHUNKS, 2)),
            pltpu.SemaphoreType.DMA((CHUNKS, 2, 3, 4)),
            pltpu.SemaphoreType.DMA((CHUNKS, 2, 3, 4)),
            pltpu.SemaphoreType.DMA((CHUNKS, 2, 3)),
            pltpu.SemaphoreType.DMA((CHUNKS, 2, 3)),
            pltpu.SemaphoreType.DMA((CHUNKS, 3)),
        ],
        compiler_params=pltpu.CompilerParams(
            collective_id=0, has_side_effects=True, vmem_limit_bytes=VMEM_LIMIT
        ),
        name="retention_step",
    )(tokens, decay.T, norm_gain.reshape(1, -1), state, w_query, w_key, w_value, w_gate, w_out)
    return layer_out, update_state(state, decayed, values, scales)


def solution(mesh):
    placed = (
        P("dp", "mp"),
        P("dp", None),
        P("dp", None, "mp"),
        P(None, "mp"),
        P(None, "mp"),
        P(None, "mp"),
        P(None, "mp"),
        P("mp", None),
        P("mp"),
    )
    return jax.shard_map(
        per_device,
        mesh=mesh,
        in_specs=placed,
        out_specs=(P("dp", "mp"), P("dp", None, "mp")),
        check_vma=False,
    )
```

```python
import functools

import jax
import jax.numpy as jnp
from jax import lax
from jax.experimental import pallas as pl
from jax.experimental.pallas import tpu as pltpu
from jax.sharding import PartitionSpec as P

HEAD = 256
VHEAD = 512
NEW = 32
EPS = 0.1
CHUNKS = 2
STEPS = 4
VMEM_LIMIT = 46 * 2**20
SIDE = 4
CHIPS = SIDE * SIDE
BLOCK = 128

MESH = pl.DeviceIdType.MESH
HIGHEST = lax.Precision.HIGHEST
BF16 = jnp.bfloat16
F32 = jnp.float32


class Place:
    def __init__(self):
        self.me = lax.axis_index("mp")
        self.core = lax.rem(self.me, 2)
        chip = lax.div(self.me, 2)
        y, x = lax.div(chip, SIDE), lax.rem(chip, SIDE)
        self.a = x * (1 - self.core) + y * self.core
        self.b = y * (1 - self.core) + x * self.core
        self.step_a = 1 + (SIDE - 1) * self.core
        self.step_b = SIDE - (SIDE - 1) * self.core
        self.partner = self.me + 1 - 2 * self.core

    def chip(self, da, db):
        a = lax.rem(self.a + (da + SIDE), SIDE)
        b = lax.rem(self.b + (db + SIDE), SIDE)
        return a * self.step_a + b * self.step_b

    def at(self, da, db):
        return self.chip(da, db) * 2 + self.core

    def partner_at(self, da, db):
        a = lax.rem(self.b + (da + SIDE), SIDE)
        b = lax.rem(self.a + (db + SIDE), SIDE)
        return (a * self.step_b + b * self.step_a) * 2 + 1 - self.core


def remote(src, dst, send_sem, recv_sem, device):
    return pltpu.make_async_remote_copy(
        src_ref=src,
        dst_ref=dst,
        send_sem=send_sem,
        recv_sem=recv_sem,
        device_id={"mp": device},
        device_id_type=MESH,
    )


def greet(place):
    barrier = pltpu.get_barrier_semaphore()
    others = (place.partner, place.at(1, 0), place.at(-1, 0), place.at(0, 1), place.at(0, -1))
    for other in others:
        pl.semaphore_signal(barrier, inc=1, device_id={"mp": other}, device_id_type=MESH)
    pl.semaphore_wait(barrier, len(others))


PAIRS = {
    1: ((-1, 0), (1, 0)),
    2: ((0, -1), (0, 1)),
    3: ((2, 0), (0, 2)),
    4: ((-1, -1), (-1, 1)),
    5: ((1, -1), (1, 1)),
    6: ((2, -1), (2, 1)),
    7: ((-1, 2), (1, 2)),
}
STEP_OF = {(0, 0): 0, (2, 2): 8} | {block: step for step, pair in PAIRS.items() for block in pair}
SEEN = [block + (half,) for block in STEP_OF if block != (0, 0) for half in range(2)]


def wrap(distance):
    return (distance + 1) % SIDE - 1


ORDER = (2, 1, -1, 0)
GROUP = 256
PAIR_NT = (((1,), (1,)), ((), ()))
PAIR_TN = (((0,), (0,)), ((), ()))


def kernel(
    tokens, decay_in, gain_in, state, w_query, w_key, w_value, w_gate, w_out,
    layer_out, new_state,
    held, decay, gain, weights, total, out_rows, cumul, final, along,
    retained, stats, other_stats, gated, own1, near1, s1, r1, s2, r2, own2,
    send_sems, recv_sems, pair_sems, side_sems, load_sems, stat_sems, gate_sems,
    far1_sems, near1_sems, far2_sems, near2_sems,
):
    place = Place()
    rows = tokens.shape[0]
    chunk = rows // CHUNKS
    sub = chunk // 2
    group = min(GROUP, chunk)
    me, core, partner = place.me, place.core, place.partner
    a_next = (place.at(1, 0), place.at(-1, 0))
    b_next = (place.at(0, 1), place.at(0, -1))

    greet(place)


    def rows_of(c, half):
        return pl.ds(c * chunk + half * sub, sub)

    def send(src, block, c, half, way, da, db):
        if way == "d":
            device, sem = partner, pair_sems.at[c, STEP_OF[da, db]]
        else:
            step = 1 if way[1] == "+" else -1
            device = place.at(*((step, 0) if way[0] == "a" else (0, step)))
            seen = (wrap(da - step), db) if way[0] == "a" else (da, wrap(db - step))
            sem = recv_sems.at[c, SEEN.index(seen + (half,))]
        remote(src, held.at[block, rows_of(c, half)], send_sems.at[0], sem, device).start()

    def own(c, ways):
        for half in range(2):
            for way in ways:
                send(tokens.at[rows_of(c, half)], me, c, half, way, 0, 0)

    def arrive(c, da, db, half):
        block = place.at(da, db)
        slot = held.at[block, rows_of(c, half)]
        remote(slot, slot, send_sems.at[0], recv_sems.at[c, SEEN.index((da, db, half))], partner).wait_recv()
        if db == 0:
            ways = ["b+", "b-", "d"]
            if (da, half) == (-1, 0):
                ways.insert(0, "a+")
            if (da, half) == (1, 1):
                ways.insert(0, "a-")
        elif (db, half) == (-1, 0):
            ways = ["b+", "d"]
        elif (db, half) == (1, 1):
            ways = ["b-", "d"]
        else:
            ways = ["d"]
        for way in ways:
            send(slot, block, c, half, way, da, db)

    def project(c, step):
        if step == 0:
            theirs, blocks = [partner], [me, partner]
        elif step in PAIRS:
            theirs = [place.partner_at(*offset) for offset in PAIRS[step]]
            blocks = [place.at(*offset) for offset in PAIRS[step]] + theirs
        else:
            theirs = [place.partner_at(2, 2)]
            blocks = [place.at(2, 2)] + theirs
        slots = held.at[pl.ds(0, len(theirs)), pl.ds(c * chunk, chunk)]
        remote(slots, slots, send_sems.at[0], pair_sems.at[c, step], partner).wait_recv()
        starts = [pl.multiple_of(block * BLOCK, BLOCK) for block in blocks]
        span = pl.ds(c * chunk, chunk)

        def body(which, carry):
            left = jnp.concatenate([held[block, span, :] for block in blocks], axis=1)
            right = jnp.concatenate([weights[which, pl.ds(start, BLOCK), :] for start in starts], axis=0)
            part = jnp.dot(left, right, preferred_element_type=F32)
            if step == 0:
                total[which, span, :] = part
            else:
                total[which, span, :] += part
            return carry

        lax.fori_loop(0, 4, body, 0, unroll=4)


    def decays():
        head = lax.div(me, 2)
        rates = jnp.log(decay[...])
        lane = lax.broadcasted_iota(jnp.int32, rates.shape, 0)
        rate = jnp.sum(jnp.where(lane == head, rates, 0.0), axis=0, keepdims=True)
        to = lax.broadcasted_iota(jnp.int32, (group, group), 0)
        at = lax.broadcasted_iota(jnp.int32, (group, group), 1)
        same = lax.div(to, NEW) == lax.div(at, NEW)
        causal = jnp.logical_and(same, at <= to).astype(F32)
        for g in range(rows // group):
            mine = rate[:, g * group : (g + 1) * group]
            mine = jnp.broadcast_to(mine, (128, group))
            span = slice(g * group, (g + 1) * group)
            cumul[span, :] = lax.dot_general(
                causal, mine, PAIR_NT, precision=HIGHEST, preferred_element_type=F32
            )
            final[span, :] = lax.dot_general(
                same.astype(F32), mine, PAIR_NT, precision=HIGHEST, preferred_element_type=F32
            )
            along[g] = lax.dot_general(
                mine[:8], causal, PAIR_NT, precision=HIGHEST, preferred_element_type=F32
            )

    def retain(g):
        span = pl.ds(g * group, group)
        query = (total[0, span, :] * HEAD ** (-0.5)).astype(BF16)
        key = total[1, span, :].astype(BF16)
        value = total[2, span, :].astype(BF16)
        to = lax.broadcasted_iota(jnp.int32, (group, group), 0)
        at = lax.broadcasted_iota(jnp.int32, (group, group), 1)
        causal = jnp.logical_and(lax.div(to, NEW) == lax.div(at, NEW), at <= to)
        c = cumul[span, :]
        wide = jnp.concatenate([c] * (group // 128), axis=1) if group > 128 else c[:, :group]
        gap = jnp.where(causal, wide - along[g, :1, :], 0.0)
        factor = jnp.where(causal, jnp.exp(gap), 0.0)
        scores = lax.dot_general(query, key, PAIR_NT, preferred_element_type=F32)
        weight = (scores * factor).astype(BF16)
        in_block = jnp.dot(weight, value, preferred_element_type=F32)
        last = final[span, :]
        carry_scale = jnp.exp(last - c)
        faded = (key.astype(F32) * jnp.concatenate([carry_scale] * 2, axis=1)).astype(BF16)
        from_scale = jnp.exp(c)
        from_scale = jnp.concatenate([from_scale] * 2, axis=1)
        last_scale = jnp.exp(last)
        last_scale = jnp.concatenate([last_scale] * 2, axis=1)
        parts = []
        for s in range(group // NEW):
            part = slice(s * NEW, (s + 1) * NEW)
            old = new_state[g * (group // NEW) + s]
            from_state = jnp.dot(query[part], old.astype(BF16), preferred_element_type=F32)
            parts.append(from_scale[part] * from_state + in_block[part])
            fresh = lax.dot_general(faded[part], value[part], PAIR_TN, preferred_element_type=F32)
            new_state[g * (group // NEW) + s] = last_scale[s * NEW : s * NEW + 1] * old + fresh
        kept = jnp.concatenate(parts, axis=0)
        retained[span, :] = kept
        first = jnp.sum(kept, axis=1, keepdims=True)
        second = jnp.sum(kept * kept, axis=1, keepdims=True)
        lanes = lax.broadcasted_iota(jnp.int32, (group, 128), 1)
        stats[span, :] = jnp.where(lanes < 64, first, second)

    def stat_copy(c):
        span = pl.ds(c * chunk, chunk)
        return remote(stats.at[span], other_stats.at[span], send_sems.at[3], stat_sems.at[c], partner)

    def share_stats(c):
        stat_copy(c).start()

    def gate_copy(c, owner):
        slot = gated.at[owner, pl.ds(c * chunk, chunk)]
        return remote(slot, slot, send_sems.at[4], gate_sems.at[c], partner)

    def gate(c):
        stat_copy(c).wait_recv()
        tile = min(chunk, 128)

        def body(index, carry):
            span = pl.ds(pl.multiple_of(c * chunk + index * tile, tile), tile)
            both = stats[span, :] + other_stats[span, :]
            centre = both[:, :1] / VHEAD
            variance = both[:, 64:65] / VHEAD - centre * centre
            normed = (retained[span, :] - centre) * lax.rsqrt(variance + EPS)
            g = total[3, span, :]
            gated[core, span, :] = (normed * gain[...] * (g / (1.0 + jnp.exp(-g)))).astype(BF16)
            return carry

        lax.fori_loop(0, chunk // tile, body, 0, unroll=2)
        gate_copy(c, core).start()


    def products(c, j, first, second):
        span = pl.ds(c * chunk, chunk)
        left = jnp.concatenate([gated[0, span, :], gated[1, span, :]], axis=1)
        right = jnp.concatenate(
            [out_rows[place.chip(ORDER[j], first)], out_rows[place.chip(ORDER[j], second)]], axis=1
        )
        return jnp.dot(left, right, preferred_element_type=F32)

    def put1(c, way, kind, j, value):
        at = (c, way, kind, j)
        s1[at] = value.astype(BF16)
        sem = far1_sems.at[c, way, j] if kind == 0 else near1_sems.at[c, j, way if kind == 2 else 1 - way]
        remote(s1.at[at], r1.at[at], send_sems.at[1], sem, b_next[way]).start()

    def put2(c, way, kind, value):
        at = (c, way, kind)
        s2[at] = value.astype(BF16)
        sem = far2_sems.at[c, way] if kind == 0 else near2_sems.at[c, way if kind == 2 else 1 - way]
        remote(s2.at[at], r2.at[at], send_sems.at[2], sem, a_next[way]).start()

    def await_into(slot, sem):
        remote(slot, slot, send_sems.at[0], sem, partner).wait_recv()

    def far(c, j):
        both = products(c, j, 2, 0)
        put1(c, 0, 0, j, both[:sub, :BLOCK])
        put1(c, 1, 0, j, both[sub:, :BLOCK])
        own1[c, j] = both[:, BLOCK:]

    def plain(c, j):
        both = products(c, j, 1, -1)
        put1(c, 0, 1, j, both[sub:, :BLOCK])
        put1(c, 1, 1, j, both[:sub, BLOCK:])
        near1[c, 0, j] = both[:sub, :BLOCK]
        near1[c, 1, j] = both[sub:, BLOCK:]

    def passing(c, j, way):
        await_into(r1.at[c, way, 0, j], far1_sems.at[c, way, j])
        put1(c, way, 2, j, near1[c, way, j] + r1[c, way, 0, j].astype(F32))

    def column(c, j, half):
        return (
            own1[c, j, pl.ds(half * sub, sub), :]
            + r1[c, half, 2, j].astype(F32)
            + r1[c, 1 - half, 1, j].astype(F32)
        )

    def await_column(c, j, half):
        await_into(r1.at[c, :, 1, j], near1_sems.at[c, j, half])

    def row_far(c, way):
        await_column(c, 0, way)
        put2(c, way, 0, column(c, 0, way))

    def row_plain(c, way):
        await_column(c, 1 + way, 1 - way)
        put2(c, way, 1, column(c, 1 + way, 1 - way))

    def row_passing(c, way):
        await_column(c, 1 + way, way)
        await_into(r2.at[c, way, 0], far2_sems.at[c, way])
        put2(c, way, 2, column(c, 1 + way, way) + r2[c, way, 0].astype(F32))

    def row_own(c, half):
        await_column(c, 3, half)
        own2[rows_of(c, half), :] = column(c, 3, half)

    def finish(c, half):
        span = rows_of(c, half)
        await_into(r2.at[c, :, 1], near2_sems.at[c, half])
        layer_out[span, :] = (
            own2[span, :] + r2[c, half, 2].astype(F32) + r2[c, 1 - half, 1].astype(F32)
        ).astype(BF16)


    mine = pl.ds(pl.multiple_of(core * BLOCK, BLOCK), BLOCK)
    own_rows = pl.ds(pl.multiple_of(core * 256, 256), 256)
    other_rows = pl.ds(pl.multiple_of((1 - core) * 256, 256), 256)
    loads = [
        pltpu.make_async_copy(tokens, held.at[me], load_sems.at[0]),
        pltpu.make_async_copy(w_query, weights.at[0, :, mine], load_sems.at[1]),
        pltpu.make_async_copy(w_key, weights.at[1, :, mine], load_sems.at[2]),
        pltpu.make_async_copy(w_value, weights.at[2], load_sems.at[3]),
        pltpu.make_async_copy(w_gate, weights.at[3], load_sems.at[4]),
    ]
    exchanged = [
        remote(w_query, weights.at[0, :, mine], side_sems.at[0], side_sems.at[1], partner),
        remote(w_key, weights.at[1, :, mine], side_sems.at[2], side_sems.at[3], partner),
    ]
    small_loads = [
        pltpu.make_async_copy(decay_in, decay, load_sems.at[7]),
        pltpu.make_async_copy(gain_in, gain, load_sems.at[8]),
    ]
    state_load = pltpu.make_async_copy(state, new_state, load_sems.at[5])
    out_sent = remote(out_rows.at[:, other_rows], out_rows.at[:, other_rows], side_sems.at[4], side_sems.at[5], partner)

    def start_out():
        for chip in range(CHIPS):
            columns = pl.ds(pl.multiple_of(chip * 2 * BLOCK + core * BLOCK, BLOCK), BLOCK)
            pltpu.make_async_copy(w_out.at[:, columns], out_rows.at[chip, own_rows], load_sems.at[6]).start()
        for chip in range(CHIPS):
            columns = pl.ds(pl.multiple_of(chip * 2 * BLOCK + (1 - core) * BLOCK, BLOCK), BLOCK)
            remote(
                w_out.at[:, columns], out_rows.at[chip, own_rows], side_sems.at[4], side_sems.at[5], partner
            ).start()

    def wait_out():
        slots = out_rows.at[:, own_rows]
        pltpu.make_async_copy(slots, slots, load_sems.at[6]).wait()
        out_sent.wait()

    own(0, ("a+", "a-"))
    own(0, ("b+", "b-"))
    own(0, ("d",))
    for load in small_loads + loads:
        load.start()
    for copy in exchanged:
        copy.start()
    state_load.start()
    own(1, ("a+", "a-"))
    own(1, ("b+", "b-"))
    own(1, ("d",))
    for load in small_loads:
        load.wait()
    decays()
    arrive(0, -1, 0, 0)
    arrive(0, 1, 0, 0)
    arrive(0, 0, -1, 0)
    arrive(0, 0, 1, 0)
    arrive(0, -1, 0, 1)
    arrive(0, 1, 0, 1)
    arrive(0, 0, 1, 1)
    arrive(0, 0, -1, 1)
    for load in loads:
        load.wait()
    for copy in exchanged:
        copy.wait()
    project(0, 0)
    project(1, 0)
    arrive(1, -1, 0, 0)
    arrive(1, 1, 0, 0)
    arrive(1, 0, -1, 0)
    arrive(1, 0, 1, 0)
    project(0, 1)
    project(0, 2)
    start_out()
    arrive(1, -1, 0, 1)
    arrive(1, 1, 0, 1)
    arrive(1, 0, 1, 1)
    arrive(1, 0, -1, 1)
    arrive(0, -1, 1, 0)
    arrive(0, 2, 0, 0)
    arrive(0, -1, -1, 0)
    arrive(0, 2, 0, 1)
    arrive(0, 1, 1, 0)
    arrive(0, 1, -1, 0)
    arrive(0, -1, 1, 1)
    arrive(1, 2, 0, 0)
    arrive(0, 0, 2, 0)
    arrive(0, 1, 1, 1)
    arrive(0, -1, -1, 1)
    arrive(1, 2, 0, 1)
    project(1, 1)
    arrive(0, 0, 2, 1)
    arrive(0, 1, -1, 1)
    project(1, 2)
    wait_out()
    arrive(1, -1, -1, 0)
    arrive(1, -1, 1, 0)
    project(0, 4)
    arrive(1, 1, -1, 0)
    arrive(1, 1, 1, 0)
    project(0, 3)
    arrive(1, -1, 1, 1)
    arrive(1, 0, 2, 0)
    project(0, 5)
    arrive(1, 1, 1, 1)
    arrive(1, -1, -1, 1)
    arrive(1, 0, 2, 1)
    arrive(1, 1, -1, 1)
    project(1, 4)
    arrive(0, 2, -1, 0)
    arrive(0, 2, 1, 0)
    project(1, 3)
    arrive(0, 2, 1, 1)
    arrive(0, -1, 2, 0)
    project(1, 5)
    arrive(0, -1, 2, 1)
    arrive(0, 2, -1, 1)
    arrive(0, 1, 2, 0)
    arrive(1, 2, 1, 0)
    arrive(1, 2, -1, 0)
    arrive(0, 1, 2, 1)
    project(0, 6)
    arrive(1, 2, 1, 1)
    arrive(1, 2, -1, 1)
    project(0, 7)
    arrive(1, -1, 2, 0)
    arrive(1, -1, 2, 1)
    arrive(1, 1, 2, 0)
    arrive(1, 1, 2, 1)
    project(1, 6)
    arrive(0, 2, 2, 0)
    arrive(0, 2, 2, 1)
    project(1, 7)
    arrive(1, 2, 2, 0)
    arrive(1, 2, 2, 1)
    project(0, 8)
    state_load.wait()
    retain(0)
    retain(1)
    share_stats(0)
    project(1, 8)
    retain(2)
    retain(3)
    share_stats(1)
    gate(0)
    gate(1)
    gate_copy(0, 1 - core).wait_recv()
    plain(0, 0)
    plain(0, 1)
    plain(0, 2)
    far(0, 0)
    gate_copy(1, 1 - core).wait_recv()
    plain(1, 0)
    plain(1, 1)
    plain(1, 2)
    far(1, 0)
    plain(0, 3)
    plain(1, 3)
    far(0, 1)
    far(1, 1)
    passing(0, 0, 0)
    passing(0, 0, 1)
    far(0, 2)
    far(1, 2)
    far(0, 3)
    far(1, 3)
    passing(1, 0, 0)
    passing(1, 0, 1)
    passing(0, 1, 0)
    passing(0, 1, 1)
    passing(1, 1, 0)
    passing(1, 1, 1)
    row_far(0, 0)
    row_far(0, 1)
    passing(0, 2, 0)
    passing(0, 2, 1)
    passing(1, 2, 0)
    passing(1, 2, 1)
    passing(0, 3, 0)
    passing(0, 3, 1)
    passing(1, 3, 0)
    passing(1, 3, 1)
    row_far(1, 0)
    row_far(1, 1)
    row_passing(0, 0)
    row_plain(0, 0)
    row_plain(1, 0)
    row_passing(0, 1)
    row_plain(0, 1)
    row_passing(1, 0)
    row_passing(1, 1)
    row_plain(1, 1)
    row_own(0, 1)
    row_own(0, 0)
    row_own(1, 1)
    finish(0, 1)
    finish(0, 0)
    row_own(1, 0)
    finish(1, 1)
    finish(1, 0)

    for sem, slots in enumerate((held.at[pl.ds(0, 2 * CHIPS - 1)], s1, s2, stats, gated.at[core])):
        remote(slots, slots, send_sems.at[sem], stat_sems.at[0], partner).wait_send()


def store_kernel(out_in, state_in, out, state, sems):
    step = state.shape[0] // STEPS
    copies = [pltpu.make_async_copy(out_in, out, sems.at[STEPS])]
    for i in range(STEPS):
        span = pl.ds(i * step, step)
        copies.append(pltpu.make_async_copy(state_in.at[span], state.at[span], sems.at[i]))
    for copy in copies:
        copy.start()
    for copy in copies:
        copy.wait()


def store(out, state):
    return pl.pallas_call(
        store_kernel,
        out_shape=(jax.ShapeDtypeStruct(out.shape, out.dtype), jax.ShapeDtypeStruct(state.shape, F32)),
        in_specs=[pl.BlockSpec(memory_space=pltpu.VMEM)] * 2,
        out_specs=(pl.BlockSpec(memory_space=pltpu.HBM),) * 2,
        scratch_shapes=[pltpu.SemaphoreType.DMA((STEPS + 1,))],
        compiler_params=pltpu.CompilerParams(vmem_limit_bytes=2**20),
        name="store",
    )(out, state)


def per_device(tokens, decay, state, w_query, w_key, w_value, w_gate, w_out, norm_gain):
    rows, features = tokens.shape[0], w_query.shape[0]
    chunk = rows // CHUNKS
    sub = chunk // 2
    group = min(GROUP, chunk)
    outside = pl.BlockSpec(memory_space=pltpu.HBM)
    inside = pl.BlockSpec(memory_space=pltpu.VMEM)
    layer_out, new_state = pl.pallas_call(
        kernel,
        out_shape=(
            pltpu.VMEM((rows, BLOCK), BF16),
            pltpu.VMEM(state.shape, F32),
        ),
        in_specs=[outside] * 9,
        out_specs=(inside,) * 2,
        scratch_shapes=[
            pltpu.VMEM((2 * CHIPS, rows, BLOCK), BF16),
            pltpu.VMEM((decay.shape[1], rows), F32),
            pltpu.VMEM((1, 256), F32),
            pltpu.VMEM((4, features, 256), BF16),
            pltpu.VMEM((4, rows, 256), F32),
            pltpu.VMEM((CHIPS, 512, BLOCK), BF16),
            pltpu.VMEM((rows, 128), F32),
            pltpu.VMEM((rows, 128), F32),
            pltpu.VMEM((rows // group, 8, group), F32),
            pltpu.VMEM((rows, 256), F32),
            pltpu.VMEM((rows, 128), F32),
            pltpu.VMEM((rows, 128), F32),
            pltpu.VMEM((2, rows, 256), BF16),
            pltpu.VMEM((CHUNKS, 4, chunk, BLOCK), F32),
            pltpu.VMEM((CHUNKS, 2, 4, sub, BLOCK), F32),
            pltpu.VMEM((CHUNKS, 2, 3, 4, sub, BLOCK), BF16),
            pltpu.VMEM((CHUNKS, 2, 3, 4, sub, BLOCK), BF16),
            pltpu.VMEM((CHUNKS, 2, 3, sub, BLOCK), BF16),
            pltpu.VMEM((CHUNKS, 2, 3, sub, BLOCK), BF16),
            pltpu.VMEM((rows, BLOCK), F32),
            pltpu.SemaphoreType.DMA((5,)),
            pltpu.SemaphoreType.DMA((CHUNKS, len(SEEN))),
            pltpu.SemaphoreType.DMA((CHUNKS, 9)),
            pltpu.SemaphoreType.DMA((6,)),
            pltpu.SemaphoreType.DMA((9,)),
            pltpu.SemaphoreType.DMA((CHUNKS,)),
            pltpu.SemaphoreType.DMA((CHUNKS,)),
            pltpu.SemaphoreType.DMA((CHUNKS, 2, 4)),
            pltpu.SemaphoreType.DMA((CHUNKS, 4, 2)),
            pltpu.SemaphoreType.DMA((CHUNKS, 2)),
            pltpu.SemaphoreType.DMA((CHUNKS, 2)),
        ],
        compiler_params=pltpu.CompilerParams(
            collective_id=0, has_side_effects=True, vmem_limit_bytes=VMEM_LIMIT
        ),
        name="retention_step",
    )(tokens, decay.T, norm_gain.reshape(1, -1), state, w_query, w_key, w_value, w_gate, w_out)
    return store(layer_out, new_state)


def solution(mesh):
    placed = (
        P("dp", "mp"),
        P("dp", None),
        P("dp", None, "mp"),
        P(None, "mp"),
        P(None, "mp"),
        P(None, "mp"),
        P(None, "mp"),
        P("mp", None),
        P("mp"),
    )
    return jax.shard_map(
        per_device,
        mesh=mesh,
        in_specs=placed,
        out_specs=(P("dp", "mp"), P("dp", None, "mp")),
        check_vma=False,
    )
```

```python
import functools

import jax
import jax.numpy as jnp
from jax import lax
from jax.experimental import pallas as pl
from jax.experimental.pallas import tpu as pltpu
from jax.sharding import PartitionSpec as P

HEAD = 256
VHEAD = 512
NEW = 32
EPS = 0.1
CHUNKS = 2
STEPS = 4
VMEM_LIMIT = 46 * 2**20
SIDE = 4
CHIPS = SIDE * SIDE
BLOCK = 128

MESH = pl.DeviceIdType.MESH
HIGHEST = lax.Precision.HIGHEST
BF16 = jnp.bfloat16
F32 = jnp.float32


class Place:
    def __init__(self):
        self.me = lax.axis_index("mp")
        self.core = lax.rem(self.me, 2)
        chip = lax.div(self.me, 2)
        y, x = lax.div(chip, SIDE), lax.rem(chip, SIDE)
        self.a = x * (1 - self.core) + y * self.core
        self.b = y * (1 - self.core) + x * self.core
        self.step_a = 1 + (SIDE - 1) * self.core
        self.step_b = SIDE - (SIDE - 1) * self.core
        self.partner = self.me + 1 - 2 * self.core

    def chip(self, da, db):
        a = lax.rem(self.a + (da + SIDE), SIDE)
        b = lax.rem(self.b + (db + SIDE), SIDE)
        return a * self.step_a + b * self.step_b

    def at(self, da, db):
        return self.chip(da, db) * 2 + self.core

    def partner_at(self, da, db):
        a = lax.rem(self.b + (da + SIDE), SIDE)
        b = lax.rem(self.a + (db + SIDE), SIDE)
        return (a * self.step_b + b * self.step_a) * 2 + 1 - self.core


def remote(src, dst, send_sem, recv_sem, device):
    return pltpu.make_async_remote_copy(
        src_ref=src,
        dst_ref=dst,
        send_sem=send_sem,
        recv_sem=recv_sem,
        device_id={"mp": device},
        device_id_type=MESH,
    )


def greet(place):
    barrier = pltpu.get_barrier_semaphore()
    others = (place.partner, place.at(1, 0), place.at(-1, 0), place.at(0, 1), place.at(0, -1))
    for other in others:
        pl.semaphore_signal(barrier, inc=1, device_id={"mp": other}, device_id_type=MESH)


def meet():
    pl.semaphore_wait(pltpu.get_barrier_semaphore(), 5)


PAIRS = {
    1: ((-1, 0), (1, 0)),
    2: ((0, -1), (0, 1)),
    3: ((2, 0), (0, 2)),
    4: ((-1, -1), (-1, 1)),
    5: ((1, -1), (1, 1)),
    6: ((2, -1), (2, 1)),
    7: ((-1, 2), (1, 2)),
}
STEP_OF = {(0, 0): 0, (2, 2): 8} | {block: step for step, pair in PAIRS.items() for block in pair}
SEEN = [block + (half,) for block in STEP_OF if block != (0, 0) for half in range(2)]


def wrap(distance):
    return (distance + 1) % SIDE - 1


ORDER = (2, 1, -1, 0)
GROUP = 256
PAIR_NT = (((1,), (1,)), ((), ()))
PAIR_TN = (((0,), (0,)), ((), ()))


def kernel(
    tokens, decay_in, gain_in, state, w_query, w_key, w_value, w_gate, w_out,
    layer_out, new_state,
    held, decay, gain, weights, total, out_rows, cumul, final, along,
    retained, stats, other_stats, gated, own1, near1, s1, r1, s2, r2, own2,
    send_sems, recv_sems, pair_sems, side_sems, load_sems, stat_sems, gate_sems,
    far1_sems, near1_sems, far2_sems, near2_sems,
):
    place = Place()
    rows = tokens.shape[0]
    chunk = rows // CHUNKS
    sub = chunk // 2
    group = min(GROUP, chunk)
    me, core, partner = place.me, place.core, place.partner
    a_next = (place.at(1, 0), place.at(-1, 0))
    b_next = (place.at(0, 1), place.at(0, -1))

    greet(place)


    def rows_of(c, half):
        return pl.ds(c * chunk + half * sub, sub)

    def send(src, block, c, half, way, da, db):
        if way == "d":
            device, sem = partner, pair_sems.at[c, STEP_OF[da, db]]
        else:
            step = 1 if way[1] == "+" else -1
            device = place.at(*((step, 0) if way[0] == "a" else (0, step)))
            seen = (wrap(da - step), db) if way[0] == "a" else (da, wrap(db - step))
            sem = recv_sems.at[c, SEEN.index(seen + (half,))]
        remote(src, held.at[block, rows_of(c, half)], send_sems.at[0], sem, device).start()

    def own(c, ways):
        for half in range(2):
            for way in ways:
                send(held.at[me, rows_of(c, half)], me, c, half, way, 0, 0)

    def arrive(c, da, db, half):
        block = place.at(da, db)
        slot = held.at[block, rows_of(c, half)]
        remote(slot, slot, send_sems.at[0], recv_sems.at[c, SEEN.index((da, db, half))], partner).wait_recv()
        if db == 0:
            ways = ["b+", "b-", "d"]
            if (da, half) == (-1, 0):
                ways.insert(0, "a+")
            if (da, half) == (1, 1):
                ways.insert(0, "a-")
        elif (db, half) == (-1, 0):
            ways = ["b+", "d"]
        elif (db, half) == (1, 1):
            ways = ["b-", "d"]
        else:
            ways = ["d"]
        for way in ways:
            send(slot, block, c, half, way, da, db)

    def project(c, step):
        if step == 0:
            theirs, blocks = [partner], [me, partner]
        elif step in PAIRS:
            theirs = [place.partner_at(*offset) for offset in PAIRS[step]]
            blocks = [place.at(*offset) for offset in PAIRS[step]] + theirs
        else:
            theirs = [place.partner_at(2, 2)]
            blocks = [place.at(2, 2)] + theirs
        slots = held.at[pl.ds(0, len(theirs)), pl.ds(c * chunk, chunk)]
        remote(slots, slots, send_sems.at[0], pair_sems.at[c, step], partner).wait_recv()
        starts = [pl.multiple_of(block * BLOCK, BLOCK) for block in blocks]
        span = pl.ds(c * chunk, chunk)

        def body(which, carry):
            left = jnp.concatenate([held[block, span, :] for block in blocks], axis=1)
            right = jnp.concatenate([weights[which, pl.ds(start, BLOCK), :] for start in starts], axis=0)
            part = jnp.dot(left, right, preferred_element_type=F32)
            if step == 0:
                total[which, span, :] = part
            else:
                total[which, span, :] += part
            return carry

        lax.fori_loop(0, 4, body, 0, unroll=4)


    def decays():
        head = lax.div(me, 2)
        rates = jnp.log(decay[...])
        lane = lax.broadcasted_iota(jnp.int32, rates.shape, 0)
        rate = jnp.sum(jnp.where(lane == head, rates, 0.0), axis=0, keepdims=True)
        to = lax.broadcasted_iota(jnp.int32, (group, group), 0)
        at = lax.broadcasted_iota(jnp.int32, (group, group), 1)
        same = lax.div(to, NEW) == lax.div(at, NEW)
        causal = jnp.logical_and(same, at <= to).astype(F32)
        for g in range(rows // group):
            mine = rate[:, g * group : (g + 1) * group]
            mine = jnp.broadcast_to(mine, (128, group))
            span = slice(g * group, (g + 1) * group)
            cumul[span, :] = lax.dot_general(
                causal, mine, PAIR_NT, precision=HIGHEST, preferred_element_type=F32
            )
            final[span, :] = lax.dot_general(
                same.astype(F32), mine, PAIR_NT, precision=HIGHEST, preferred_element_type=F32
            )
            along[g] = lax.dot_general(
                mine[:8], causal, PAIR_NT, precision=HIGHEST, preferred_element_type=F32
            )

    def retain(g):
        span = pl.ds(g * group, group)
        query = (total[0, span, :] * HEAD ** (-0.5)).astype(BF16)
        key = total[1, span, :].astype(BF16)
        value = total[2, span, :].astype(BF16)
        to = lax.broadcasted_iota(jnp.int32, (group, group), 0)
        at = lax.broadcasted_iota(jnp.int32, (group, group), 1)
        causal = jnp.logical_and(lax.div(to, NEW) == lax.div(at, NEW), at <= to)
        c = cumul[span, :]
        wide = jnp.concatenate([c] * (group // 128), axis=1) if group > 128 else c[:, :group]
        gap = jnp.where(causal, wide - along[g, :1, :], 0.0)
        factor = jnp.where(causal, jnp.exp(gap), 0.0)
        scores = lax.dot_general(query, key, PAIR_NT, preferred_element_type=F32)
        weight = (scores * factor).astype(BF16)
        in_block = jnp.dot(weight, value, preferred_element_type=F32)
        last = final[span, :]
        carry_scale = jnp.exp(last - c)
        faded = (key.astype(F32) * jnp.concatenate([carry_scale] * 2, axis=1)).astype(BF16)
        from_scale = jnp.exp(c)
        from_scale = jnp.concatenate([from_scale] * 2, axis=1)
        last_scale = jnp.exp(last)
        last_scale = jnp.concatenate([last_scale] * 2, axis=1)
        parts = []
        for s in range(group // NEW):
            part = slice(s * NEW, (s + 1) * NEW)
            old = new_state[g * (group // NEW) + s]
            from_state = jnp.dot(query[part], old.astype(BF16), preferred_element_type=F32)
            parts.append(from_scale[part] * from_state + in_block[part])
            fresh = lax.dot_general(faded[part], value[part], PAIR_TN, preferred_element_type=F32)
            new_state[g * (group // NEW) + s] = last_scale[s * NEW : s * NEW + 1] * old + fresh
        kept = jnp.concatenate(parts, axis=0)
        retained[span, :] = kept
        first = jnp.sum(kept, axis=1, keepdims=True)
        second = jnp.sum(kept * kept, axis=1, keepdims=True)
        lanes = lax.broadcasted_iota(jnp.int32, (group, 128), 1)
        stats[span, :] = jnp.where(lanes < 64, first, second)

    def stat_copy(c):
        span = pl.ds(c * chunk, chunk)
        return remote(stats.at[span], other_stats.at[span], send_sems.at[3], stat_sems.at[c], partner)

    def share_stats(c):
        stat_copy(c).start()

    def gate_copy(c, owner):
        slot = gated.at[owner, pl.ds(c * chunk, chunk)]
        return remote(slot, slot, send_sems.at[4], gate_sems.at[c], partner)

    def gate(c):
        stat_copy(c).wait_recv()
        tile = min(chunk, 128)

        def body(index, carry):
            span = pl.ds(pl.multiple_of(c * chunk + index * tile, tile), tile)
            both = stats[span, :] + other_stats[span, :]
            centre = both[:, :1] / VHEAD
            variance = both[:, 64:65] / VHEAD - centre * centre
            normed = (retained[span, :] - centre) * lax.rsqrt(variance + EPS)
            g = total[3, span, :]
            gated[core, span, :] = (normed * gain[...] * (g / (1.0 + jnp.exp(-g)))).astype(BF16)
            return carry

        lax.fori_loop(0, chunk // tile, body, 0, unroll=2)
        gate_copy(c, core).start()


    def products(c, j, first, second):
        span = pl.ds(c * chunk, chunk)
        left = jnp.concatenate([gated[0, span, :], gated[1, span, :]], axis=1)
        right = jnp.concatenate(
            [out_rows[place.chip(ORDER[j], first)], out_rows[place.chip(ORDER[j], second)]], axis=1
        )
        return jnp.dot(left, right, preferred_element_type=F32)

    def put1(c, way, kind, j, value):
        at = (c, way, kind, j)
        s1[at] = value.astype(BF16)
        sem = far1_sems.at[c, way, j] if kind == 0 else near1_sems.at[c, j, way if kind == 2 else 1 - way]
        remote(s1.at[at], r1.at[at], send_sems.at[1], sem, b_next[way]).start()

    def put2(c, way, kind, value):
        at = (c, way, kind)
        s2[at] = value.astype(BF16)
        sem = far2_sems.at[c, way] if kind == 0 else near2_sems.at[c, way if kind == 2 else 1 - way]
        remote(s2.at[at], r2.at[at], send_sems.at[2], sem, a_next[way]).start()

    def await_into(slot, sem):
        remote(slot, slot, send_sems.at[0], sem, partner).wait_recv()

    def far(c, j):
        both = products(c, j, 2, 0)
        put1(c, 0, 0, j, both[:sub, :BLOCK])
        put1(c, 1, 0, j, both[sub:, :BLOCK])
        own1[c, j] = both[:, BLOCK:]

    def plain(c, j):
        both = products(c, j, 1, -1)
        put1(c, 0, 1, j, both[sub:, :BLOCK])
        put1(c, 1, 1, j, both[:sub, BLOCK:])
        near1[c, 0, j] = both[:sub, :BLOCK]
        near1[c, 1, j] = both[sub:, BLOCK:]

    def passing(c, j, way):
        await_into(r1.at[c, way, 0, j], far1_sems.at[c, way, j])
        put1(c, way, 2, j, near1[c, way, j] + r1[c, way, 0, j].astype(F32))

    def column(c, j, half):
        return (
            own1[c, j, pl.ds(half * sub, sub), :]
            + r1[c, half, 2, j].astype(F32)
            + r1[c, 1 - half, 1, j].astype(F32)
        )

    def await_column(c, j, half):
        await_into(r1.at[c, :, 1, j], near1_sems.at[c, j, half])

    def row_far(c, way):
        await_column(c, 0, way)
        put2(c, way, 0, column(c, 0, way))

    def row_plain(c, way):
        await_column(c, 1 + way, 1 - way)
        put2(c, way, 1, column(c, 1 + way, 1 - way))

    def row_passing(c, way):
        await_column(c, 1 + way, way)
        await_into(r2.at[c, way, 0], far2_sems.at[c, way])
        put2(c, way, 2, column(c, 1 + way, way) + r2[c, way, 0].astype(F32))

    def row_own(c, half):
        await_column(c, 3, half)
        own2[rows_of(c, half), :] = column(c, 3, half)

    def finish(c, half):
        span = rows_of(c, half)
        await_into(r2.at[c, :, 1], near2_sems.at[c, half])
        layer_out[span, :] = (
            own2[span, :] + r2[c, half, 2].astype(F32) + r2[c, 1 - half, 1].astype(F32)
        ).astype(BF16)


    mine = pl.ds(pl.multiple_of(core * BLOCK, BLOCK), BLOCK)
    own_rows = pl.ds(pl.multiple_of(core * 256, 256), 256)
    other_rows = pl.ds(pl.multiple_of((1 - core) * 256, 256), 256)
    loads = [
        pltpu.make_async_copy(w_query, weights.at[0, :, mine], load_sems.at[1]),
        pltpu.make_async_copy(w_key, weights.at[1, :, mine], load_sems.at[2]),
        pltpu.make_async_copy(w_value, weights.at[2], load_sems.at[3]),
        pltpu.make_async_copy(w_gate, weights.at[3], load_sems.at[4]),
    ]
    exchanged = [
        remote(w_query, weights.at[0, :, mine], side_sems.at[0], side_sems.at[1], partner),
        remote(w_key, weights.at[1, :, mine], side_sems.at[2], side_sems.at[3], partner),
    ]
    token_load = pltpu.make_async_copy(tokens, held.at[me], load_sems.at[0])
    small_loads = [
        pltpu.make_async_copy(decay_in, decay, load_sems.at[7]),
        pltpu.make_async_copy(gain_in, gain, load_sems.at[8]),
    ]
    state_load = pltpu.make_async_copy(state, new_state, load_sems.at[5])
    out_sent = remote(out_rows.at[:, other_rows], out_rows.at[:, other_rows], side_sems.at[4], side_sems.at[5], partner)

    def start_out():
        for chip in range(CHIPS):
            columns = pl.ds(pl.multiple_of(chip * 2 * BLOCK + core * BLOCK, BLOCK), BLOCK)
            pltpu.make_async_copy(w_out.at[:, columns], out_rows.at[chip, own_rows], load_sems.at[6]).start()
        for chip in range(CHIPS):
            columns = pl.ds(pl.multiple_of(chip * 2 * BLOCK + (1 - core) * BLOCK, BLOCK), BLOCK)
            remote(
                w_out.at[:, columns], out_rows.at[chip, own_rows], side_sems.at[4], side_sems.at[5], partner
            ).start()

    def wait_out():
        slots = out_rows.at[:, own_rows]
        pltpu.make_async_copy(slots, slots, load_sems.at[6]).wait()
        out_sent.wait()

    for load in [token_load] + small_loads + loads:
        load.start()
    state_load.start()
    token_load.wait()
    meet()
    own(0, ("a+", "a-"))
    own(0, ("b+", "b-"))
    own(0, ("d",))
    for copy in exchanged:
        copy.start()
    for load in small_loads:
        load.wait()
    decays()
    arrive(0, -1, 0, 0)
    arrive(0, 1, 0, 0)
    arrive(0, 0, -1, 0)
    arrive(0, 0, 1, 0)
    arrive(0, -1, 0, 1)
    arrive(0, 1, 0, 1)
    arrive(0, 0, 1, 1)
    arrive(0, 0, -1, 1)
    own(1, ("d",))
    arrive(0, -1, 1, 0)
    for load in loads:
        load.wait()
    for copy in exchanged:
        copy.wait()
    start_out()
    project(0, 0)
    arrive(0, 2, 0, 0)
    arrive(0, -1, -1, 0)
    arrive(0, 1, 1, 0)
    project(1, 0)
    arrive(0, 1, -1, 0)
    project(0, 1)
    arrive(0, 2, 0, 1)
    arrive(0, -1, 1, 1)
    arrive(0, 0, 2, 0)
    project(0, 2)
    arrive(0, 1, 1, 1)
    arrive(0, -1, -1, 1)
    arrive(0, 0, 2, 1)
    own(1, ("a+", "a-"))
    arrive(0, 1, -1, 1)
    arrive(0, 2, -1, 0)
    arrive(0, 2, 1, 0)
    project(0, 4)
    arrive(0, 2, 1, 1)
    arrive(0, -1, 2, 0)
    wait_out()
    own(1, ("b+", "b-"))
    project(0, 3)
    project(0, 5)
    arrive(0, -1, 2, 1)
    arrive(0, 1, 2, 0)
    arrive(1, -1, 0, 0)
    arrive(1, 1, 0, 0)
    arrive(0, 1, 2, 1)
    arrive(0, 2, -1, 1)
    arrive(1, -1, 0, 1)
    arrive(1, 1, 0, 1)
    arrive(0, 2, 2, 0)
    arrive(0, 2, 2, 1)
    project(0, 7)
    project(0, 6)
    arrive(1, 0, -1, 0)
    arrive(1, 0, 1, 0)
    project(1, 1)
    arrive(1, 2, 0, 0)
    arrive(1, 0, 1, 1)
    project(0, 8)
    arrive(1, 0, -1, 1)
    state_load.wait()
    retain(0)
    arrive(1, -1, -1, 0)
    arrive(1, -1, 1, 0)
    arrive(1, 2, 0, 1)
    retain(1)
    arrive(1, 1, -1, 0)
    arrive(1, 1, 1, 0)
    share_stats(0)
    project(1, 2)
    arrive(1, -1, 1, 1)
    arrive(1, -1, -1, 1)
    arrive(1, 1, 1, 1)
    arrive(1, 1, -1, 1)
    gate(0)
    arrive(1, 0, 2, 0)
    arrive(1, 2, 1, 0)
    project(1, 4)
    arrive(1, 2, -1, 0)
    arrive(1, 0, 2, 1)
    project(1, 5)
    arrive(1, 2, 1, 1)
    arrive(1, -1, 2, 0)
    gate_copy(0, 1 - core).wait_recv()
    far(0, 0)
    arrive(1, -1, 2, 1)
    arrive(1, 2, -1, 1)
    far(0, 1)
    far(0, 2)
    arrive(1, 1, 2, 0)
    arrive(1, 1, 2, 1)
    far(0, 3)
    arrive(1, 2, 2, 0)
    plain(0, 0)
    arrive(1, 2, 2, 1)
    plain(0, 1)
    plain(0, 2)
    passing(0, 0, 0)
    passing(0, 0, 1)
    project(1, 3)
    passing(0, 1, 0)
    passing(0, 1, 1)
    project(1, 6)
    project(1, 7)
    project(1, 8)
    retain(2)
    retain(3)
    share_stats(1)
    passing(0, 2, 0)
    passing(0, 2, 1)
    plain(0, 3)
    passing(0, 3, 0)
    passing(0, 3, 1)
    row_far(0, 0)
    row_far(0, 1)
    gate(1)
    row_plain(0, 0)
    row_plain(0, 1)
    gate_copy(1, 1 - core).wait_recv()
    far(1, 0)
    far(1, 1)
    far(1, 2)
    far(1, 3)
    row_own(0, 0)
    row_own(0, 1)
    plain(1, 0)
    plain(1, 1)
    plain(1, 2)
    passing(1, 0, 0)
    passing(1, 0, 1)
    plain(1, 3)
    passing(1, 1, 0)
    passing(1, 1, 1)
    row_passing(0, 0)
    row_passing(0, 1)
    passing(1, 2, 0)
    passing(1, 2, 1)
    passing(1, 3, 0)
    passing(1, 3, 1)
    finish(0, 0)
    finish(0, 1)
    row_far(1, 0)
    row_far(1, 1)
    row_plain(1, 0)
    row_plain(1, 1)
    row_passing(1, 0)
    row_passing(1, 1)
    row_own(1, 1)
    row_own(1, 0)
    finish(1, 0)
    finish(1, 1)

    for sem, slots in enumerate((held.at[pl.ds(0, 2 * CHIPS - 1)], s1, s2, stats, gated.at[core])):
        remote(slots, slots, send_sems.at[sem], stat_sems.at[0], partner).wait_send()


def store_kernel(out_in, state_in, out, state, sems):
    step = state.shape[0] // STEPS
    copies = [pltpu.make_async_copy(out_in, out, sems.at[STEPS])]
    for i in range(STEPS):
        span = pl.ds(i * step, step)
        copies.append(pltpu.make_async_copy(state_in.at[span], state.at[span], sems.at[i]))
    for copy in copies:
        copy.start()
    for copy in copies:
        copy.wait()


def store(out, state):
    return pl.pallas_call(
        store_kernel,
        out_shape=(jax.ShapeDtypeStruct(out.shape, out.dtype), jax.ShapeDtypeStruct(state.shape, F32)),
        in_specs=[pl.BlockSpec(memory_space=pltpu.VMEM)] * 2,
        out_specs=(pl.BlockSpec(memory_space=pltpu.HBM),) * 2,
        scratch_shapes=[pltpu.SemaphoreType.DMA((STEPS + 1,))],
        compiler_params=pltpu.CompilerParams(vmem_limit_bytes=2**20),
        name="store",
    )(out, state)


def per_device(tokens, decay, state, w_query, w_key, w_value, w_gate, w_out, norm_gain):
    rows, features = tokens.shape[0], w_query.shape[0]
    chunk = rows // CHUNKS
    sub = chunk // 2
    group = min(GROUP, chunk)
    outside = pl.BlockSpec(memory_space=pltpu.HBM)
    inside = pl.BlockSpec(memory_space=pltpu.VMEM)
    layer_out, new_state = pl.pallas_call(
        kernel,
        out_shape=(
            pltpu.VMEM((rows, BLOCK), BF16),
            pltpu.VMEM(state.shape, F32),
        ),
        in_specs=[outside] * 9,
        out_specs=(inside,) * 2,
        scratch_shapes=[
            pltpu.VMEM((2 * CHIPS, rows, BLOCK), BF16),
            pltpu.VMEM((decay.shape[1], rows), F32),
            pltpu.VMEM((1, 256), F32),
            pltpu.VMEM((4, features, 256), BF16),
            pltpu.VMEM((4, rows, 256), F32),
            pltpu.VMEM((CHIPS, 512, BLOCK), BF16),
            pltpu.VMEM((rows, 128), F32),
            pltpu.VMEM((rows, 128), F32),
            pltpu.VMEM((rows // group, 8, group), F32),
            pltpu.VMEM((rows, 256), F32),
            pltpu.VMEM((rows, 128), F32),
            pltpu.VMEM((rows, 128), F32),
            pltpu.VMEM((2, rows, 256), BF16),
            pltpu.VMEM((CHUNKS, 4, chunk, BLOCK), F32),
            pltpu.VMEM((CHUNKS, 2, 4, sub, BLOCK), F32),
            pltpu.VMEM((CHUNKS, 2, 3, 4, sub, BLOCK), BF16),
            pltpu.VMEM((CHUNKS, 2, 3, 4, sub, BLOCK), BF16),
            pltpu.VMEM((CHUNKS, 2, 3, sub, BLOCK), BF16),
            pltpu.VMEM((CHUNKS, 2, 3, sub, BLOCK), BF16),
            pltpu.VMEM((rows, BLOCK), F32),
            pltpu.SemaphoreType.DMA((5,)),
            pltpu.SemaphoreType.DMA((CHUNKS, len(SEEN))),
            pltpu.SemaphoreType.DMA((CHUNKS, 9)),
            pltpu.SemaphoreType.DMA((6,)),
            pltpu.SemaphoreType.DMA((9,)),
            pltpu.SemaphoreType.DMA((CHUNKS,)),
            pltpu.SemaphoreType.DMA((CHUNKS,)),
            pltpu.SemaphoreType.DMA((CHUNKS, 2, 4)),
            pltpu.SemaphoreType.DMA((CHUNKS, 4, 2)),
            pltpu.SemaphoreType.DMA((CHUNKS, 2)),
            pltpu.SemaphoreType.DMA((CHUNKS, 2)),
        ],
        compiler_params=pltpu.CompilerParams(
            collective_id=0, has_side_effects=True, vmem_limit_bytes=VMEM_LIMIT
        ),
        name="retention_step",
    )(tokens, decay.T, norm_gain.reshape(1, -1), state, w_query, w_key, w_value, w_gate, w_out)
    return store(layer_out, new_state)


def solution(mesh):
    placed = (
        P("dp", "mp"),
        P("dp", None),
        P("dp", None, "mp"),
        P(None, "mp"),
        P(None, "mp"),
        P(None, "mp"),
        P(None, "mp"),
        P("mp", None),
        P("mp"),
    )
    return jax.shard_map(
        per_device,
        mesh=mesh,
        in_specs=placed,
        out_specs=(P("dp", "mp"), P("dp", None, "mp")),
        check_vma=False,
    )
```
